32 devices in a mesh: row: 4 (over y, core), col: 8 (over z, x).
Axes of the slice: x: 2, y: 2, z: 4, core: 2. Of those that a mesh axis runs over, the one named last changes fastest.
Arguments:
- factors: bfloat16 [32, 2, 512, 512], P(('row', 'col')), as said below
- target: int32 [64, 1], P(('row', 'col')), may hold values from 0 to 31; in each aligned block of 64 rows (0 to 63, 64 to 127, ...) at most 3 rows name the same one
Outputs:
- roots: float32 [32, 3, 512, 512], P(('row', 'col'))
The draws below stay inside these ranges and needn't reach their ends.
Inputs may be any that keep to these rules, and one draw needn't show every extreme that they name: `factors`: every block is symmetric and positive definite. `target`: every device receives between 1 and 3 blocks; some device receives exactly 3.
All inputs are finite; a program needn't handle non-finite values.
Results may differ from the reference program's by a relative error of at most 0.0003.
Values may be sent and summed in bfloat16 or wider, within the bound.
No kernel may reach another device: no remote copies, remote signals or barrier semaphores. Data moves between devices by JAX's collectives and lax.ppermute only.
A program may use at most 128 MiB of HBM per device.

```python
import math
import jax
import jax.numpy as jnp
import numpy as np
from jax import lax

BW = 512
HOLD = 2
ITERS = 3
CAP = 3
N_ROW = 4
N_COL = 8


def draw_factors(key, part):
    key_noise, key_diag, key_scale = jax.random.split(key, 3)
    block_total = N_ROW * N_COL * HOLD
    noise = jax.random.normal(key_noise, (block_total, BW, BW), jnp.float32)
    diagonal = jnp.exp(jax.random.uniform(key_diag, (block_total, BW), jnp.float32, 0.0, math.log(10.0)))
    symmetric = (noise + jnp.swapaxes(noise, 1, 2)) / math.sqrt(2.0)
    inner = jnp.eye(BW, dtype=jnp.float32)[None] + 0.4 / math.sqrt(BW) * symmetric
    half_diag = jnp.sqrt(diagonal)
    blocks = half_diag[:, :, None] * inner * half_diag[:, None, :]
    column = jnp.arange(block_total) // HOLD % N_COL
    rising = 1.0 + 2.0 * column.astype(jnp.float32) / max(N_COL - 1, 1)
    jitter = jnp.exp(jax.random.uniform(key_scale, (block_total,), jnp.float32, math.log(0.8), math.log(1.25)))
    blocks = blocks * (rising * jitter)[:, None, None]
    return blocks.reshape(N_ROW * N_COL, HOLD, BW, BW).astype(jnp.bfloat16)


def assign_block(own_key, own, number, rows, count, top, reach, slope):
    order = jax.random.permutation(own_key, count)
    heavy_load, common = shares(count, rows * top, reach, slope, True), shares(count, rows * top, reach, slope, False)
    places = jnp.arange(count)

    def named(tallies, rotation):
        used = int((tallies > 0).sum())
        fixed = max(1, used // 4)
        moved = fixed + (places - fixed + rotation * (used - fixed)) % max(1, count - fixed)
        return jnp.zeros((count,), jnp.int32).at[order[jnp.where(places < fixed, places, moved)]].set(jnp.asarray(tallies, jnp.int32))

    tallies = jnp.where(number % 4 == 0, named(heavy_load, number // 4), named(common, number - number // 4 - 1))
    mixed = jax.random.permutation(jax.random.fold_in(own, 3), count)
    giver, sink = mixed[0:count // 2 * 2:2], mixed[1:count // 2 * 2:2]
    room = jnp.minimum(tallies[giver] - 1, reach - tallies[sink]) // 2
    room = jnp.where((giver == order[0]) | (sink == order[0]) | (tallies[sink] == 0), 0, jnp.maximum(room, 0))
    moved = jax.random.randint(jax.random.fold_in(own, 4), (count // 2,), 0, 1 << 20) % (room + 1)
    tallies = tallies.at[giver].add(-moved).at[sink].add(moved)
    items = jnp.searchsorted(jnp.cumsum(tallies), jnp.arange(rows * top), side="right").astype(jnp.int32)
    listing = items.reshape(top, rows).T
    listing = listing[jax.random.permutation(jax.random.fold_in(own, 1), rows)]
    rotation = jax.random.randint(jax.random.fold_in(own, 2), (rows, 1), 0, top)
    return jnp.take_along_axis(listing, (jnp.arange(top)[None, :] + rotation) % top, axis=1)


def shares(count, total, limit, slope, full):
    loads = [(1 << 20) // math.isqrt(rank ** slope) + 1 for rank in range(1, count + 1)]
    largest = limit if full else min(limit, max(-(-total // count), total * loads[0] // sum(loads)))
    least = 1 if total - largest >= count - 1 else 0
    counts, surplus = [largest] + [least] * (count - 1), total - largest - least * (count - 1)
    while surplus > 0:
        candidates = [i for i in range(1, count) if counts[i] < largest] or [i for i in range(1, count) if counts[i] < limit]
        pool, remaining = sum([loads[i] for i in candidates]), surplus
        for i in candidates:
            more = min(limit - counts[i], max(1, remaining * loads[i] // pool), surplus)
            counts[i] = counts[i] + more
            surplus = surplus - more
    return np.array(counts)


def setup_inputs(seed: int = 0) -> dict:
    key_list = jax.random.split(jax.random.key(seed), 3)
    factors = draw_factors(jax.random.fold_in(key_list[2], 71), 0)
    target_keys = jax.random.split(jax.random.fold_in(key_list[1], 1), (N_ROW * N_COL * HOLD) // (N_ROW * N_COL * HOLD))
    target_turns = jax.random.permutation(jax.random.fold_in(key_list[1], 3), (N_ROW * N_COL * HOLD) // (N_ROW * N_COL * HOLD))
    target = jax.vmap(lambda own, number: assign_block(jax.random.fold_in(key_list[1], 2), own, number, N_ROW * N_COL * HOLD, N_ROW * N_COL, 1, CAP, 2))(target_keys, target_turns).reshape((N_ROW * N_COL * HOLD, 1))
    return dict(factors=factors, target=target)


HIGH = lax.Precision.HIGHEST

def newton_root(block, scale):
    identity = jnp.eye(BW, dtype=jnp.float32)
    moment = block / scale
    root_iter = identity
    for repeat in range(ITERS):
        step_mat = 1.25 * identity - 0.25 * moment
        square_mat = jnp.dot(step_mat, step_mat, precision=HIGH)
        fourth_mat = jnp.dot(square_mat, square_mat, precision=HIGH)
        moment = jnp.dot(fourth_mat, moment, precision=HIGH)
        root_iter = jnp.dot(root_iter, step_mat, precision=HIGH)
    return root_iter * scale ** (-0.25)

def reference(factors, target):
    block_total = N_ROW * N_COL * HOLD
    blocks = factors.reshape(block_total, BW, BW).astype(jnp.float32)
    block_sq = lax.optimization_barrier(jnp.sum(blocks * blocks, axis=(1, 2)))
    source_rows = jnp.arange(block_total, dtype=jnp.int32) // (N_COL * HOLD)
    layer_totals = lax.optimization_barrier(jnp.sum(block_sq.reshape(N_ROW, N_COL * HOLD), axis=1))
    scales = 2.0 * jnp.sqrt(layer_totals[source_rows] / (N_COL * HOLD * BW))
    results = lax.map(lambda operands: newton_root(operands[0], operands[1]), (blocks, scales))
    targets = target[:, 0].astype(jnp.int32)
    peer_ids = jnp.arange(N_ROW * N_COL, dtype=jnp.int32)
    matches = (targets[:, None] == peer_ids[None, :]).astype(jnp.int32)
    slot_index = lax.optimization_barrier(jnp.sum((jnp.cumsum(matches, axis=0) - matches) * matches, axis=1)).astype(jnp.int32)
    output = jnp.zeros((N_ROW * N_COL, CAP, BW, BW), jnp.float32)
    return output.at[targets, slot_index].set(results)
```

```python
import functools
import jax
import jax.numpy as jnp
from jax import lax
from jax.experimental import pallas as pl
from jax.experimental.pallas import tpu as pltpu
from jax.sharding import PartitionSpec as P

CAP = 3
LANE = 128
INFO_ROWS = 8
AXES = ("row", "col")


def pack_kernel(pieces, target_ref, block_ref, packed_ref, info_ref):
    hold, width = block_ref.shape[1], block_ref.shape[2]
    half = width // 2
    depth = packed_ref.shape[2]
    row_ids = lax.broadcasted_iota(jnp.int32, (half, half), 0)
    col_ids = lax.broadcasted_iota(jnp.int32, (half, half), 1)
    info = jnp.zeros((INFO_ROWS, LANE), jnp.float32)
    info_row = lax.broadcasted_iota(jnp.int32, (INFO_ROWS, LANE), 0)
    info_col = lax.broadcasted_iota(jnp.int32, (INFO_ROWS, LANE), 1)
    square_sum = jnp.zeros((1, 1), jnp.float32)
    chunks = half // LANE
    for slot in range(hold):
        upper = block_ref[0, slot, :half, :half].astype(jnp.float32)
        corner = block_ref[0, slot, half:, :half]
        lower = block_ref[0, slot, half:, half:].astype(jnp.float32)
        wide = corner.astype(jnp.float32)
        folded = upper * upper + lower * lower + 2.0 * (wide * wide)
        square_sum = square_sum + jnp.sum(jnp.sum(folded, axis=0, keepdims=True), axis=1, keepdims=True)
        diagonal = jnp.sum(jnp.where(row_ids == col_ids, lower, 0.0), axis=0, keepdims=True)
        mixed = jnp.where(row_ids >= col_ids, upper, lower).astype(jnp.bfloat16)
        stripes = [corner[:, c * LANE:(c + 1) * LANE] for c in range(chunks)]
        stripes += [mixed[:, c * LANE:(c + 1) * LANE] for c in range(chunks)]
        per_stripe = half // depth
        for piece in range(pieces):
            stripe, place = piece // per_stripe, piece % per_stripe
            packed_ref[piece, slot] = stripes[stripe][place * depth:(place + 1) * depth]
        for c in range(chunks):
            line = diagonal[:, c * LANE:(c + 1) * LANE]
            info = jnp.where(info_row == slot * chunks + c, line, info)
    tail = info_row == hold * chunks
    info = jnp.where(tail & (info_col == 0), square_sum, info)
    for slot in range(hold):
        name = target_ref[slot, 0].astype(jnp.float32)
        info = jnp.where(tail & (info_col == 1 + slot), name, info)
    for piece in range(pieces):
        info_ref[piece] = info


def pack(factors, target, pieces):
    hold, width = factors.shape[1], factors.shape[2]
    depth = width * width // 2 // LANE // pieces
    return pl.pallas_call(
        functools.partial(pack_kernel, pieces),
        out_shape=(
            jax.ShapeDtypeStruct((pieces, hold, depth, LANE), jnp.bfloat16),
            jax.ShapeDtypeStruct((pieces, INFO_ROWS, LANE), jnp.float32),
        ),
        in_specs=[
            pl.BlockSpec(memory_space=pltpu.SMEM),
            pl.BlockSpec(memory_space=pltpu.VMEM),
        ],
        name="pack",
    )(target, factors)


def select_kernel(index_ref, pieces_ref, *out_refs):
    for slot, out_ref in enumerate(out_refs):
        for owner in range(out_ref.shape[0]):
            out_ref[owner] = pieces_ref[index_ref[slot, owner]]


def select(index, pieces):
    owners = index.shape[1]
    shape = jax.ShapeDtypeStruct((owners,) + pieces.shape[1:], pieces.dtype)
    return pl.pallas_call(
        select_kernel,
        out_shape=(shape,) * CAP,
        in_specs=[
            pl.BlockSpec(memory_space=pltpu.SMEM),
            pl.BlockSpec(memory_space=pltpu.VMEM),
        ],
        name="select",
    )(index, pieces)


def split(value):
    high = value.astype(jnp.bfloat16)
    return high, (value - high.astype(jnp.float32)).astype(jnp.bfloat16)


def dot(left, right):
    return jnp.dot(left, right, preferred_element_type=jnp.float32)


def product(left, right):
    return dot(
        jnp.concatenate([left[0], left[1], left[0]], axis=1),
        jnp.concatenate([right[0], right[0], right[1]], axis=0),
    )


def root_kernel(param_ref, packed_ref, diagonal_ref, *rest):
    out_ref, block_ref = rest[-2], rest[-1]
    width = out_ref.shape[1]
    half = width // 2
    chunks = half // LANE

    @pl.when(param_ref[0] > 0.0)
    def _():
        def square(first):
            return jnp.concatenate(
                [packed_ref[pl.ds((first + c) * half, half), :] for c in range(chunks)], axis=1
            )

        corner = square(0)
        mixed = square(chunks).astype(jnp.float32)
        turned = mixed.T
        row_ids = lax.broadcasted_iota(jnp.int32, (half, half), 0)
        col_ids = lax.broadcasted_iota(jnp.int32, (half, half), 1)
        upper = jnp.where(row_ids >= col_ids, mixed, turned)
        lower = jnp.where(row_ids < col_ids, mixed, turned)
        lower = jnp.where(row_ids == col_ids, diagonal_ref[...], lower)
        block_ref[:half, :half] = upper.astype(jnp.bfloat16)
        block_ref[:half, half:] = corner.astype(jnp.float32).T.astype(jnp.bfloat16)
        block_ref[half:, :half] = corner
        block_ref[half:, half:] = lower.astype(jnp.bfloat16)
        inverse = param_ref[1]
        block = block_ref[...]
        wide = block.astype(jnp.float32)
        rows = lax.broadcasted_iota(jnp.int32, (width, width), 0)
        cols = lax.broadcasted_iota(jnp.int32, (width, width), 1)
        eye = rows == cols
        step = jnp.where(eye, 1.25, 0.0) - (0.25 * inverse) * wide
        block_square = dot(block, block)
        step_square = (
            jnp.where(eye, 1.5625, 0.0)
            - (0.625 * inverse) * wide
            + (0.0625 * inverse * inverse) * block_square
        )
        parts = split(step_square)
        step_fourth = product(parts, parts)
        inner = split(step_square - 1.25 * step)
        pair = 1.25 * step + product(split(step_fourth), inner)
        pair_parts = split(pair)
        pair_square = split(product(pair_parts, pair_parts))
        pair_fourth = split(product(pair_square, pair_square))
        tail = dot(
            jnp.concatenate(pair_fourth, axis=1), jnp.concatenate([block, block], axis=0)
        )
        last = jnp.where(eye, 1.25, 0.0) - (0.25 * inverse) * tail
        out_ref[0] = product(pair_parts, split(last)) * param_ref[2]

    @pl.when(param_ref[0] <= 0.0)
    def _():
        out_ref[...] = jnp.zeros_like(out_ref)


def root(params, packed, diagonal, slot, width, held):
    shape = jax.ShapeDtypeStruct((CAP, width, width), jnp.float32)
    operands = [params, packed, diagonal]
    in_specs = [
        pl.BlockSpec(memory_space=pltpu.SMEM),
        pl.BlockSpec(memory_space=pltpu.VMEM),
        pl.BlockSpec(memory_space=pltpu.VMEM),
    ]
    aliases = {}
    if held is not None:
        operands.append(held)
        in_specs.append(pl.BlockSpec(memory_space=pl.ANY))
        aliases = {3: 0}
    return pl.pallas_call(
        root_kernel,
        grid=(1,),
        out_shape=shape,
        in_specs=in_specs,
        out_specs=pl.BlockSpec((1, width, width), lambda i: (slot, 0, 0)),
        scratch_shapes=[pltpu.VMEM((width, width), jnp.bfloat16)],
        input_output_aliases=aliases,
        cost_estimate=pl.CostEstimate(
            flops=36 * width ** 3, bytes_accessed=5 * width * width, transcendentals=0
        ),
        name="root",
    )(*operands)


def shards(factors, target):
    row_count, col_count = lax.axis_size("row"), lax.axis_size("col")
    devices = row_count * col_count
    hold, width = factors.shape[1], factors.shape[2]
    total = devices * hold
    me = lax.axis_index("row") * col_count + lax.axis_index("col")
    packed, info = pack(factors, target, devices)
    info = lax.all_to_all(info, AXES, split_axis=0, concat_axis=0, tiled=True)
    pieces = lax.all_to_all(packed, AXES, split_axis=0, concat_axis=0, tiled=True)
    lines = hold * width // 2 // LANE
    targets = info[:, lines, 1:1 + hold].reshape(total).astype(jnp.int32)
    squares = info[:, lines, 0].reshape(row_count, col_count)
    scales = 2.0 * jnp.sqrt(jnp.sum(squares, axis=1) / (col_count * hold * width))
    numbers = jnp.arange(total, dtype=jnp.int32)
    same = targets[:, None] == targets[None, :]
    slots = jnp.sum((same & (numbers[None, :] < numbers[:, None])).astype(jnp.int32), axis=1)
    places = jnp.arange(CAP * devices, dtype=jnp.int32)
    wanted = (slots * devices + targets)[None, :] == places[:, None]
    index = jnp.sum(jnp.where(wanted, numbers[None, :], 0), axis=1).reshape(CAP, devices)
    mine = (slots[None, :] == jnp.arange(CAP)[:, None]) & (targets[None, :] == me)
    valid = jnp.sum(mine.astype(jnp.float32), axis=1)
    per_block = jnp.repeat(scales, col_count * hold)
    scale = jnp.sum(jnp.where(mine, per_block[None, :], 0.0), axis=1)
    scale = jnp.where(valid > 0, scale, 1.0)
    params = jnp.stack([valid, 1.0 / scale, scale ** (-0.25)], axis=1)
    diagonals = info[:, :lines].reshape(total, width // 2)
    diagonal = jnp.sum(jnp.where(mine[:, :, None], diagonals[None], 0.0), axis=1)
    chosen = select(index, pieces.reshape((total,) + pieces.shape[2:]))
    held = None
    for slot in range(CAP):
        landed = lax.all_to_all(chosen[slot], AXES, split_axis=0, concat_axis=0, tiled=True)
        held = root(
            params[slot], landed.reshape(-1, LANE), diagonal[slot][None], slot, width, held
        )
    return held[None]


def solution(mesh):
    return jax.shard_map(
        shards,
        mesh=mesh,
        in_specs=(P(AXES, None, None, None), P(AXES, None)),
        out_specs=P(AXES, None, None, None),
        check_vma=False,
    )
```

```python
import functools
import jax
import jax.numpy as jnp
from jax import lax
from jax.experimental import pallas as pl
from jax.experimental.pallas import tpu as pltpu
from jax.sharding import PartitionSpec as P

CAP = 3
LANE = 128
INFO_ROWS = 8
SQUARE_PARTS = 3
NAME_PARTS = 2
EARLY = 2
AXES = ("row", "col")


def parts_of(value, count):
    parts = []
    for _ in range(count):
        part = value.astype(jnp.bfloat16)
        parts.append(part)
        value = value - part.astype(jnp.float32)
    return parts


def pack_kernel(pieces, target_ref, block_ref, packed_ref):
    hold, width = block_ref.shape[1], block_ref.shape[2]
    half = width // 2
    depth = (packed_ref.shape[1] - INFO_ROWS) // hold
    row_ids = lax.broadcasted_iota(jnp.int32, (half, half), 0)
    col_ids = lax.broadcasted_iota(jnp.int32, (half, half), 1)
    info = jnp.zeros((INFO_ROWS, LANE), jnp.float32)
    info_row = lax.broadcasted_iota(jnp.int32, (INFO_ROWS, LANE), 0)
    info_col = lax.broadcasted_iota(jnp.int32, (INFO_ROWS, LANE), 1)
    square_sum = jnp.zeros((1, 1), jnp.float32)
    chunks = half // LANE
    for slot in range(hold):
        upper = block_ref[0, slot, :half, :half].astype(jnp.float32)
        corner = block_ref[0, slot, half:, :half]
        lower = block_ref[0, slot, half:, half:].astype(jnp.float32)
        wide = corner.astype(jnp.float32)
        folded = upper * upper + lower * lower + 2.0 * (wide * wide)
        square_sum = square_sum + jnp.sum(jnp.sum(folded, axis=0, keepdims=True), axis=1, keepdims=True)
        diagonal = jnp.sum(jnp.where(row_ids == col_ids, lower, 0.0), axis=0, keepdims=True)
        mixed = jnp.where(row_ids >= col_ids, upper, lower).astype(jnp.bfloat16)
        stripes = [corner[:, c * LANE:(c + 1) * LANE] for c in range(chunks)]
        stripes += [mixed[:, c * LANE:(c + 1) * LANE] for c in range(chunks)]
        per_stripe = half // depth
        for piece in range(pieces):
            stripe, place = piece // per_stripe, piece % per_stripe
            packed_ref[piece, slot * depth:(slot + 1) * depth] = (
                stripes[stripe][place * depth:(place + 1) * depth]
            )
        for c in range(chunks):
            line = diagonal[:, c * LANE:(c + 1) * LANE]
            info = jnp.where(info_row == slot * chunks + c, line, info)
    tail = info_row == hold * chunks
    values = parts_of(square_sum, SQUARE_PARTS)
    for slot in range(hold):
        name = jnp.zeros((1, 1), jnp.float32) + target_ref[slot, 0].astype(jnp.float32)
        values += parts_of(name, NAME_PARTS)
    for place, value in enumerate(values):
        info = jnp.where(tail & (info_col == place), value.astype(jnp.float32), info)
    info = info.astype(jnp.bfloat16)
    for piece in range(pieces):
        packed_ref[piece, hold * depth:] = info


def pack(factors, target, pieces):
    hold, width = factors.shape[1], factors.shape[2]
    depth = width * width // 2 // LANE // pieces
    return pl.pallas_call(
        functools.partial(pack_kernel, pieces),
        out_shape=jax.ShapeDtypeStruct((pieces, hold * depth + INFO_ROWS, LANE), jnp.bfloat16),
        in_specs=[
            pl.BlockSpec(memory_space=pltpu.SMEM),
            pl.BlockSpec(memory_space=pltpu.VMEM),
        ],
        name="pack",
    )(target, factors)


def select_kernel(hold, index_ref, pieces_ref, early_ref, late_ref):
    early, depth = early_ref.shape[1], early_ref.shape[2]
    for owner in range(early_ref.shape[0]):
        for slot in range(CAP):
            block = index_ref[slot, owner]
            first = pl.multiple_of((block % hold) * depth, depth)
            piece = pieces_ref[block // hold, pl.ds(first, depth), :]
            if slot < early:
                early_ref[owner, slot] = piece
            else:
                late_ref[owner, slot - early] = piece


def select(index, pieces, hold):
    owners = index.shape[1]
    depth = (pieces.shape[1] - INFO_ROWS) // hold
    return pl.pallas_call(
        functools.partial(select_kernel, hold),
        out_shape=(
            jax.ShapeDtypeStruct((owners, EARLY, depth, LANE), pieces.dtype),
            jax.ShapeDtypeStruct((owners, CAP - EARLY, depth, LANE), pieces.dtype),
        ),
        in_specs=[
            pl.BlockSpec(memory_space=pltpu.SMEM),
            pl.BlockSpec(memory_space=pltpu.VMEM),
        ],
        name="select",
    )(index, pieces)


def split(value):
    high = value.astype(jnp.bfloat16)
    return high, (value - high.astype(jnp.float32)).astype(jnp.bfloat16)


def dot(left, right):
    return jnp.dot(left, right, preferred_element_type=jnp.float32)


def product(left, right):
    return dot(
        jnp.concatenate([left[0], left[1], left[0]], axis=1),
        jnp.concatenate([right[0], right[0], right[1]], axis=0),
    )


def root_kernel(first, param_ref, packed_ref, diagonal_ref, *rest):
    out_ref, block_ref = rest[-2], rest[-1]
    width = out_ref.shape[1]
    half = width // 2
    chunks = half // LANE
    owners, depth = packed_ref.shape[0], packed_ref.shape[2]
    here = pl.program_id(0)
    slot = first + here
    lines = packed_ref[:, here].reshape(owners * depth, LANE)

    def square(place):
        return jnp.concatenate(
            [lines[(place + c) * half:(place + c + 1) * half] for c in range(chunks)], axis=1
        )

    corner = square(0)
    mixed = square(chunks).astype(jnp.float32)
    turned = mixed.T
    row_ids = lax.broadcasted_iota(jnp.int32, (half, half), 0)
    col_ids = lax.broadcasted_iota(jnp.int32, (half, half), 1)
    upper = jnp.where(row_ids >= col_ids, mixed, turned)
    lower = jnp.where(row_ids < col_ids, mixed, turned)
    lower = jnp.where(row_ids == col_ids, diagonal_ref[pl.ds(slot, 1), :], lower)
    block_ref[:half, :half] = upper.astype(jnp.bfloat16)
    block_ref[:half, half:] = corner.astype(jnp.float32).T.astype(jnp.bfloat16)
    block_ref[half:, :half] = corner
    block_ref[half:, half:] = lower.astype(jnp.bfloat16)
    inverse = param_ref[slot, 1]
    block = block_ref[...]
    wide = block.astype(jnp.float32)
    rows = lax.broadcasted_iota(jnp.int32, (width, width), 0)
    cols = lax.broadcasted_iota(jnp.int32, (width, width), 1)
    eye = rows == cols
    step = jnp.where(eye, 1.25, 0.0) - (0.25 * inverse) * wide
    block_square = dot(block, block)
    step_square = (
        jnp.where(eye, 1.5625, 0.0)
        - (0.625 * inverse) * wide
        + (0.0625 * inverse * inverse) * block_square
    )
    parts = split(step_square)
    step_fourth = product(parts, parts)
    inner = split(step_square - 1.25 * step)
    pair = 1.25 * step + product(split(step_fourth), inner)
    pair_parts = split(pair)
    pair_square = split(product(pair_parts, pair_parts))
    pair_fourth = split(product(pair_square, pair_square))
    tail = dot(jnp.concatenate(pair_fourth, axis=1), jnp.concatenate([block, block], axis=0))
    last = jnp.where(eye, 1.25, 0.0) - (0.25 * inverse) * tail
    result = product(pair_parts, split(last)) * param_ref[slot, 2]
    out_ref[0] = jnp.where(param_ref[slot, 0] > 0.0, result, 0.0)


def root(params, packed, diagonal, first, width, held):
    count = packed.shape[1]
    operands = [params, packed, diagonal]
    in_specs = [
        pl.BlockSpec(memory_space=pltpu.SMEM),
        pl.BlockSpec(memory_space=pltpu.VMEM),
        pl.BlockSpec(memory_space=pltpu.VMEM),
    ]
    aliases = {}
    if held is not None:
        operands.append(held)
        in_specs.append(pl.BlockSpec(memory_space=pl.ANY))
        aliases = {3: 0}
    return pl.pallas_call(
        functools.partial(root_kernel, first),
        grid=(count,),
        out_shape=jax.ShapeDtypeStruct((CAP, width, width), jnp.float32),
        in_specs=in_specs,
        out_specs=pl.BlockSpec((1, width, width), lambda i: (first + i, 0, 0)),
        scratch_shapes=[pltpu.VMEM((width, width), jnp.bfloat16)],
        input_output_aliases=aliases,
        cost_estimate=pl.CostEstimate(
            flops=36 * count * width ** 3,
            bytes_accessed=5 * count * width * width,
            transcendentals=0,
        ),
        name="root",
    )(*operands)


def shards(factors, target):
    row_count, col_count = lax.axis_size("row"), lax.axis_size("col")
    devices = row_count * col_count
    hold, width = factors.shape[1], factors.shape[2]
    total = devices * hold
    me = lax.axis_index("row") * col_count + lax.axis_index("col")
    packed = pack(factors, target, devices)
    pieces = lax.all_to_all(packed, AXES, split_axis=0, concat_axis=0, tiled=True)
    lines = hold * width // 2 // LANE
    info = pieces[:, -INFO_ROWS:].astype(jnp.float32)
    tail = info[:, lines]
    named = tail[:, SQUARE_PARTS:SQUARE_PARTS + hold * NAME_PARTS]
    targets = jnp.sum(named.reshape(total, NAME_PARTS), axis=1).astype(jnp.int32)
    squares = jnp.sum(tail[:, :SQUARE_PARTS], axis=1).reshape(row_count, col_count)
    scales = 2.0 * jnp.sqrt(jnp.sum(squares, axis=1) / (col_count * hold * width))
    numbers = jnp.arange(total, dtype=jnp.int32)
    same = targets[:, None] == targets[None, :]
    slots = jnp.sum((same & (numbers[None, :] < numbers[:, None])).astype(jnp.int32), axis=1)
    places = jnp.arange(CAP * devices, dtype=jnp.int32)
    wanted = (slots * devices + targets)[None, :] == places[:, None]
    index = jnp.sum(jnp.where(wanted, numbers[None, :], 0), axis=1).reshape(CAP, devices)
    mine = (slots[None, :] == jnp.arange(CAP)[:, None]) & (targets[None, :] == me)
    valid = jnp.sum(mine.astype(jnp.float32), axis=1)
    per_block = jnp.repeat(scales, col_count * hold)
    scale = jnp.sum(jnp.where(mine, per_block[None, :], 0.0), axis=1)
    scale = jnp.where(valid > 0, scale, 1.0)
    params = jnp.stack([valid, 1.0 / scale, scale ** (-0.25)], axis=1)
    diagonals = info[:, :lines].reshape(total, width // 2)
    diagonal = jnp.sum(jnp.where(mine[:, :, None], diagonals[None], 0.0), axis=1)
    early, late = select(index, pieces, hold)
    early = lax.all_to_all(early, AXES, split_axis=0, concat_axis=0, tiled=True)
    late = lax.all_to_all(late, AXES, split_axis=0, concat_axis=0, tiled=True)
    held = root(params, early, diagonal, 0, width, None)
    return root(params, late, diagonal, EARLY, width, held)[None]


def solution(mesh):
    return jax.shard_map(
        shards,
        mesh=mesh,
        in_specs=(P(AXES, None, None, None), P(AXES, None)),
        out_specs=P(AXES, None, None, None),
        check_vma=False,
    )
```

```python
import functools
import jax
import jax.numpy as jnp
from jax import lax
from jax.experimental import pallas as pl
from jax.experimental.pallas import tpu as pltpu
from jax.sharding import PartitionSpec as P

CAP = 3
LANE = 128
INFO_ROWS = 8
SQUARE_PARTS = 3
NAME_PARTS = 2
EARLY = 2
AXES = ("row", "col")


def parts_of(value, count):
    parts = []
    for _ in range(count):
        part = value.astype(jnp.bfloat16)
        parts.append(part)
        value = value - part.astype(jnp.float32)
    return parts


def pack_kernel(pieces, target_ref, block_ref, packed_ref):
    hold, width = block_ref.shape[1], block_ref.shape[2]
    half = width // 2
    depth = (packed_ref.shape[1] - INFO_ROWS) // hold
    row_ids = lax.broadcasted_iota(jnp.int32, (half, half), 0)
    col_ids = lax.broadcasted_iota(jnp.int32, (half, half), 1)
    info = jnp.zeros((INFO_ROWS, LANE), jnp.float32)
    info_row = lax.broadcasted_iota(jnp.int32, (INFO_ROWS, LANE), 0)
    info_col = lax.broadcasted_iota(jnp.int32, (INFO_ROWS, LANE), 1)
    square_sum = jnp.zeros((1, 1), jnp.float32)
    chunks = half // LANE
    for slot in range(hold):
        upper = block_ref[0, slot, :half, :half].astype(jnp.float32)
        corner = block_ref[0, slot, half:, :half]
        lower = block_ref[0, slot, half:, half:].astype(jnp.float32)
        wide = corner.astype(jnp.float32)
        folded = upper * upper + lower * lower + 2.0 * (wide * wide)
        square_sum = square_sum + jnp.sum(jnp.sum(folded, axis=0, keepdims=True), axis=1, keepdims=True)
        diagonal = jnp.sum(jnp.where(row_ids == col_ids, lower, 0.0), axis=0, keepdims=True)
        mixed = jnp.where(row_ids >= col_ids, upper, lower).astype(jnp.bfloat16)
        stripes = [corner[:, c * LANE:(c + 1) * LANE] for c in range(chunks)]
        stripes += [mixed[:, c * LANE:(c + 1) * LANE] for c in range(chunks)]
        per_stripe = half // depth
        for piece in range(pieces):
            stripe, place = piece // per_stripe, piece % per_stripe
            packed_ref[piece, slot * depth:(slot + 1) * depth] = (
                stripes[stripe][place * depth:(place + 1) * depth]
            )
        for c in range(chunks):
            line = diagonal[:, c * LANE:(c + 1) * LANE]
            info = jnp.where(info_row == slot * chunks + c, line, info)
    tail = info_row == hold * chunks
    values = parts_of(square_sum, SQUARE_PARTS)
    for slot in range(hold):
        name = jnp.zeros((1, 1), jnp.float32) + target_ref[0, slot].astype(jnp.float32)
        values += parts_of(name, NAME_PARTS)
    for place, value in enumerate(values):
        info = jnp.where(tail & (info_col == place), value.astype(jnp.float32), info)
    info = info.astype(jnp.bfloat16)
    for piece in range(pieces):
        packed_ref[piece, hold * depth:] = info


def pack(factors, target, pieces):
    hold, width = factors.shape[1], factors.shape[2]
    depth = width * width // 2 // LANE // pieces
    return pl.pallas_call(
        functools.partial(pack_kernel, pieces),
        out_shape=pltpu.VMEM((pieces, hold * depth + INFO_ROWS, LANE), jnp.bfloat16),
        in_specs=[
            pl.BlockSpec(memory_space=pltpu.SMEM),
            pl.BlockSpec(memory_space=pltpu.VMEM),
        ],
        out_specs=pl.BlockSpec(memory_space=pltpu.VMEM),
        name="pack",
    )(target.T, factors)


def select_kernel(hold, name_ref, pieces_ref, chosen_ref, count_ref):
    depth = chosen_ref.shape[2]
    for owner in range(chosen_ref.shape[0]):
        count_ref[owner] = 0
    for block in range(name_ref.shape[0]):
        owner = name_ref[block]
        slot = count_ref[owner]
        count_ref[owner] = slot + 1
        first = (block % hold) * depth
        chosen_ref[owner, slot] = pieces_ref[block // hold, first:first + depth]


def select(names, pieces, hold, owners):
    depth = (pieces.shape[1] - INFO_ROWS) // hold
    return pl.pallas_call(
        functools.partial(select_kernel, hold),
        out_shape=pltpu.VMEM((owners, CAP, depth, LANE), pieces.dtype),
        in_specs=[
            pl.BlockSpec(memory_space=pltpu.SMEM),
            pl.BlockSpec(memory_space=pltpu.VMEM),
        ],
        out_specs=pl.BlockSpec(memory_space=pltpu.VMEM),
        scratch_shapes=[pltpu.SMEM((owners,), jnp.int32)],
        name="select",
    )(names, pltpu.with_memory_space_constraint(pieces, pltpu.VMEM))


def split(value):
    high = value.astype(jnp.bfloat16)
    return high, (value - high.astype(jnp.float32)).astype(jnp.bfloat16)


def dot(left, right):
    return jnp.dot(left, right, preferred_element_type=jnp.float32)


def root_kernel(first, param_ref, packed_ref, diagonal_ref, *rest):
    out_ref, block_ref, high_ref, low_ref = rest[-4:]
    count, width = out_ref.shape[0], out_ref.shape[1]
    half = width // 2
    chunks = half // LANE
    full, top, bottom = slice(0, width), slice(0, half), slice(half, width)
    tiles = ((top, top), (bottom, top), (bottom, bottom))
    row_ids = lax.broadcasted_iota(jnp.int32, (half, half), 0)
    col_ids = lax.broadcasted_iota(jnp.int32, (half, half), 1)
    eye = row_ids == col_ids
    slots = range(count)

    def add_eye(values, scalar):
        there = jnp.where(eye, scalar, 0.0)
        return values[0] + there, values[1], values[2] + there

    def store(slot, place, values):
        for tile, value in zip(tiles, values):
            high, low = split(value)
            high_ref[slot, place, tile[0], tile[1]] = high
            low_ref[slot, place, tile[0], tile[1]] = low
            if tile == (bottom, top):
                high_ref[slot, place, top, bottom] = high.T
                low_ref[slot, place, top, bottom] = low.T

    def dots(left, right):
        def some(rows, cols):
            return dot(
                jnp.concatenate([part(rows, full) for part in left], axis=1),
                jnp.concatenate([part(full, cols) for part in right], axis=0),
            )

        lower = some(bottom, full)
        return some(top, top), lower[:, top], lower[:, bottom]

    def at(ref, *place):
        return lambda rows, cols: ref[place + (rows, cols)]

    def product(slot, left, right):
        high, low = at(high_ref, slot, left), at(low_ref, slot, left)
        return dots(
            [high, low, high],
            [at(high_ref, slot, right), at(high_ref, slot, right), at(low_ref, slot, right)],
        )

    def by_block(slot, left):
        block = at(block_ref, slot)
        return dots([at(high_ref, slot, left), at(low_ref, slot, left)], [block, block])

    def block_tiles(slot):
        return [block_ref[slot, rows, cols].astype(jnp.float32) for rows, cols in tiles]

    inverses = [param_ref[first + slot, 1] for slot in slots]
    for slot in slots:
        lines = packed_ref[:, slot].reshape(-1, LANE)

        def square(place):
            return jnp.concatenate(
                [lines[(place + c) * half:(place + c + 1) * half] for c in range(chunks)], axis=1
            )

        corner = square(0)
        mixed = square(chunks).astype(jnp.float32)
        turned = mixed.T
        upper = jnp.where(row_ids >= col_ids, mixed, turned)
        lower = jnp.where(row_ids < col_ids, mixed, turned)
        lower = jnp.where(eye, diagonal_ref[first + slot:first + slot + 1, :], lower)
        block_ref[slot, top, top] = upper.astype(jnp.bfloat16)
        block_ref[slot, bottom, top] = corner
        block_ref[slot, top, bottom] = corner.T
        block_ref[slot, bottom, bottom] = lower.astype(jnp.bfloat16)
    for slot in slots:
        scaled = [(0.25 * inverses[slot]) * tile for tile in block_tiles(slot)]
        squared = dots([at(block_ref, slot)], [at(block_ref, slot)])
        factor = 0.0625 * inverses[slot] * inverses[slot]
        store(
            slot, 0, add_eye([factor * b - 2.5 * a for a, b in zip(scaled, squared)], 1.5625)
        )
    def tile_sum(slot, place):
        return [
            high_ref[slot, place, rows, cols].astype(jnp.float32)
            + low_ref[slot, place, rows, cols].astype(jnp.float32)
            for rows, cols in tiles
        ]

    for slot in slots:
        turned = by_block(slot, 0)
        squares = tile_sum(slot, 0)
        cubes = [1.25 * a - (0.25 * inverses[slot]) * b for a, b in zip(squares, turned)]
        store(slot, 1, cubes)
        store(slot, 2, [a - 1.25 * b for a, b in zip(cubes, squares)])
    for slot in slots:
        sixth = product(slot, 1, 2)
        scaled = [(0.3125 * inverses[slot]) * tile for tile in block_tiles(slot)]
        store(slot, 0, add_eye([b - a for a, b in zip(scaled, sixth)], 1.5625))
    for slot in slots:
        store(slot, 1, product(slot, 0, 0))
    for slot in slots:
        store(slot, 2, product(slot, 1, 1))
    for slot in slots:
        tail = by_block(slot, 2)
        store(slot, 1, add_eye([-(0.25 * inverses[slot]) * tile for tile in tail], 1.25))
    for slot in slots:
        result = product(slot, 0, 1)
        valid = param_ref[first + slot, 0] > 0.0
        result = [jnp.where(valid, tile * param_ref[first + slot, 2], 0.0) for tile in result]
        for (rows, cols), tile in zip(tiles, result):
            out_ref[slot, rows, cols] = tile
        out_ref[slot, top, bottom] = result[1].T


def root(params, packed, diagonal, first, width, held):
    count = packed.shape[1]
    operands = [params, pltpu.with_memory_space_constraint(packed, pltpu.VMEM), diagonal]
    in_specs = [
        pl.BlockSpec(memory_space=pltpu.SMEM),
        pl.BlockSpec(memory_space=pltpu.VMEM),
        pl.BlockSpec(memory_space=pltpu.VMEM),
    ]
    aliases = {}
    if held is not None:
        operands.append(held)
        in_specs.append(pl.BlockSpec(memory_space=pl.ANY))
        aliases = {3: 0}
    return pl.pallas_call(
        functools.partial(root_kernel, first),
        grid=(1,),
        out_shape=jax.ShapeDtypeStruct((CAP, width, width), jnp.float32),
        in_specs=in_specs,
        out_specs=pl.BlockSpec((count, width, width), lambda i: (first // count, 0, 0)),
        scratch_shapes=[
            pltpu.VMEM((count, width, width), jnp.bfloat16),
            pltpu.VMEM((count, 3, width, width), jnp.bfloat16),
            pltpu.VMEM((count, 3, width, width), jnp.bfloat16),
        ],
        input_output_aliases=aliases,
        cost_estimate=pl.CostEstimate(
            flops=36 * count * width ** 3,
            bytes_accessed=5 * count * width * width,
            transcendentals=0,
        ),
        name="root",
    )(*operands)


def shards(factors, target):
    row_count, col_count = lax.axis_size("row"), lax.axis_size("col")
    devices = row_count * col_count
    hold, width = factors.shape[1], factors.shape[2]
    total = devices * hold
    me = lax.axis_index("row") * col_count + lax.axis_index("col")
    packed = pack(factors, target, devices)
    pieces = lax.all_to_all(packed, AXES, split_axis=0, concat_axis=0, tiled=True)
    lines = hold * width // 2 // LANE
    info = pieces[:, -INFO_ROWS:].astype(jnp.float32)
    tail = info[:, lines]
    named = tail[:, SQUARE_PARTS:SQUARE_PARTS + hold * NAME_PARTS]
    targets = jnp.sum(named.reshape(total, NAME_PARTS), axis=1).astype(jnp.int32)
    squares = jnp.sum(tail[:, :SQUARE_PARTS], axis=1).reshape(row_count, col_count)
    scales = 2.0 * jnp.sqrt(jnp.sum(squares, axis=1) / (col_count * hold * width))
    numbers = jnp.arange(total, dtype=jnp.int32)
    same = targets[:, None] == targets[None, :]
    slots = jnp.sum((same & (numbers[None, :] < numbers[:, None])).astype(jnp.int32), axis=1)
    mine = (slots[None, :] == jnp.arange(CAP)[:, None]) & (targets[None, :] == me)
    valid = jnp.sum(mine.astype(jnp.float32), axis=1)
    per_block = jnp.repeat(scales, col_count * hold)
    scale = jnp.sum(jnp.where(mine, per_block[None, :], 0.0), axis=1)
    scale = jnp.where(valid > 0, scale, 1.0)
    params = jnp.stack([valid, 1.0 / scale, scale ** (-0.25)], axis=1)
    diagonals = info[:, :lines].reshape(total, width // 2)
    diagonal = jnp.sum(jnp.where(mine[:, :, None], diagonals[None], 0.0), axis=1)
    chosen = select(targets, pieces, hold, devices)
    landed = lax.all_to_all(chosen, AXES, split_axis=0, concat_axis=0, tiled=True)
    return root(params, landed, diagonal, 0, width, None)[None]


def solution(mesh):
    return jax.shard_map(
        shards,
        mesh=mesh,
        in_specs=(P(AXES, None, None, None), P(AXES, None)),
        out_specs=P(AXES, None, None, None),
        check_vma=False,
    )
```

```python
import functools
import jax
import jax.numpy as jnp
from jax import lax
from jax.experimental import pallas as pl
from jax.experimental.pallas import tpu as pltpu
from jax.sharding import PartitionSpec as P

CAP = 3
LANE = 128
INFO_ROWS = 8
SQUARE_PARTS = 3
NAME_PARTS = 2
AXES = ("row", "col")
RING = ("col", "row")


def parts_of(value, count):
    parts = []
    for _ in range(count):
        part = value.astype(jnp.bfloat16)
        parts.append(part)
        value = value - part.astype(jnp.float32)
    return parts


def pack_kernel(row_count, col_count, target_ref, block_ref, packed_ref):
    hold, width = block_ref.shape[1], block_ref.shape[2]
    pieces = packed_ref.shape[0]
    half = width // 2
    depth = (packed_ref.shape[1] - INFO_ROWS) // hold
    row_ids = lax.broadcasted_iota(jnp.int32, (half, half), 0)
    col_ids = lax.broadcasted_iota(jnp.int32, (half, half), 1)
    info = jnp.zeros((INFO_ROWS, LANE), jnp.float32)
    info_row = lax.broadcasted_iota(jnp.int32, (INFO_ROWS, LANE), 0)
    info_col = lax.broadcasted_iota(jnp.int32, (INFO_ROWS, LANE), 1)
    square_sum = jnp.zeros((1, 1), jnp.float32)
    chunks = half // LANE
    for slot in range(hold):
        upper = block_ref[0, slot, :half, :half].astype(jnp.float32)
        corner = block_ref[0, slot, half:, :half]
        lower = block_ref[0, slot, half:, half:].astype(jnp.float32)
        wide = corner.astype(jnp.float32)
        folded = upper * upper + lower * lower + 2.0 * (wide * wide)
        square_sum = square_sum + jnp.sum(jnp.sum(folded, axis=0, keepdims=True), axis=1, keepdims=True)
        diagonal = jnp.sum(jnp.where(row_ids == col_ids, lower, 0.0), axis=0, keepdims=True)
        mixed = jnp.where(row_ids >= col_ids, upper, lower).astype(jnp.bfloat16)
        stripes = [corner[:, c * LANE:(c + 1) * LANE] for c in range(chunks)]
        stripes += [mixed[:, c * LANE:(c + 1) * LANE] for c in range(chunks)]
        per_stripe = half // depth
        for piece in range(pieces):
            stripe, place = piece // per_stripe, piece % per_stripe
            packed_ref[piece, slot * depth:(slot + 1) * depth] = (
                stripes[stripe][place * depth:(place + 1) * depth]
            )
        for c in range(chunks):
            line = diagonal[:, c * LANE:(c + 1) * LANE]
            info = jnp.where(info_row == slot * chunks + c, line, info)
    tail = info_row == hold * chunks
    values = parts_of(square_sum, SQUARE_PARTS)
    for slot in range(hold):
        owner = target_ref[0, slot]
        place = lax.rem(owner, col_count) * row_count + lax.div(owner, col_count)
        place = jnp.zeros((1, 1), jnp.float32) + place.astype(jnp.float32)
        values += parts_of(place, NAME_PARTS)
    for place, value in enumerate(values):
        info = jnp.where(tail & (info_col == place), value.astype(jnp.float32), info)
    info = info.astype(jnp.bfloat16)
    for piece in range(pieces):
        packed_ref[piece, hold * depth:] = info


def pack(factors, target, row_count, col_count):
    hold, width = factors.shape[1], factors.shape[2]
    pieces = row_count * col_count
    depth = width * width // 2 // LANE // pieces
    return pl.pallas_call(
        functools.partial(pack_kernel, row_count, col_count),
        out_shape=pltpu.VMEM((pieces, hold * depth + INFO_ROWS, LANE), jnp.bfloat16),
        in_specs=[
            pl.BlockSpec(memory_space=pltpu.SMEM),
            pl.BlockSpec(memory_space=pltpu.VMEM),
        ],
        out_specs=pl.BlockSpec(memory_space=pltpu.VMEM),
        name="pack",
    )(target.T, factors)


def select_kernel(
    hold, row_count, col_count, width, pieces_ref, chosen_ref, param_ref,
    name_ref, place_ref, count_ref, table_ref, sem,
):
    owners, depth = chosen_ref.shape[0], chosen_ref.shape[2]
    rows = hold * depth
    half_lines = width // 2 // LANE
    info = pieces_ref[:, rows:rows + INFO_ROWS].astype(jnp.float32)
    tail = info[:, hold * half_lines]
    names = [tail]
    for part in range(1, NAME_PARTS):
        names.append(pltpu.roll(tail, LANE - part, 1))
    name_ref[...] = sum(names).astype(jnp.int32)
    copy = pltpu.make_async_copy(name_ref, place_ref, sem)
    copy.start()
    for owner in range(owners):
        count_ref[owner] = 0
    copy.wait()
    for device in range(owners):
        source = (device % col_count) * row_count + device // col_count
        for part in range(hold):
            owner = place_ref[source, SQUARE_PARTS + part * NAME_PARTS]
            slot = count_ref[owner]
            count_ref[owner] = slot + 1
            table_ref[owner, slot] = source * hold + part
            chosen_ref[owner, slot] = pieces_ref[source, part * depth:(part + 1) * depth]
    me = lax.axis_index("col") * row_count + lax.axis_index("row")
    source_ids = lax.broadcasted_iota(jnp.int32, (owners, LANE), 0)
    lanes = lax.broadcasted_iota(jnp.int32, (owners, LANE), 1)
    squares = jnp.where(lanes < SQUARE_PARTS, tail, 0.0)
    for slot in range(CAP):
        valid = slot < count_ref[me]
        code = jnp.where(valid, table_ref[me, slot], 0)
        source, part = lax.div(code, hold), lax.rem(code, hold)
        same_row = lax.rem(source_ids, row_count) == lax.rem(source, row_count)
        total = jnp.sum(
            jnp.sum(jnp.where(same_row, squares, 0.0), axis=0, keepdims=True), axis=1, keepdims=True
        )
        scale = 2.0 * jnp.sqrt(total / (col_count * hold * width))
        inverse = 1.0 / scale
        gain = lax.rsqrt(jnp.sqrt(scale))
        here = pieces_ref[source, rows:rows + INFO_ROWS].astype(jnp.float32)
        diagonal = here[:half_lines]
        for other in range(1, hold):
            lines = here[other * half_lines:(other + 1) * half_lines]
            diagonal = jnp.where(part == other, lines, diagonal)
        param_ref[slot, :half_lines] = diagonal
        one = jnp.zeros((1, LANE), jnp.float32)
        param_ref[slot, half_lines:half_lines + 1] = one + inverse
        param_ref[slot, half_lines + 1:half_lines + 2] = jnp.where(valid, one + gain, 0.0)


def select(pieces, hold, row_count, col_count, width):
    owners = pieces.shape[0]
    depth = (pieces.shape[1] - INFO_ROWS) // hold
    return pl.pallas_call(
        functools.partial(select_kernel, hold, row_count, col_count, width),
        out_shape=(
            pltpu.VMEM((owners, CAP, depth, LANE), pieces.dtype),
            pltpu.VMEM((CAP, INFO_ROWS, LANE), jnp.float32),
        ),
        in_specs=[pl.BlockSpec(memory_space=pltpu.VMEM)],
        out_specs=(
            pl.BlockSpec(memory_space=pltpu.VMEM),
            pl.BlockSpec(memory_space=pltpu.VMEM),
        ),
        scratch_shapes=[
            pltpu.VMEM((owners, LANE), jnp.int32),
            pltpu.SMEM((owners, LANE), jnp.int32),
            pltpu.SMEM((owners,), jnp.int32),
            pltpu.SMEM((owners, CAP), jnp.int32),
            pltpu.SemaphoreType.DMA,
        ],
        name="select",
    )(pltpu.with_memory_space_constraint(pieces, pltpu.VMEM))


def split(value):
    high = value.astype(jnp.bfloat16)
    return high, (value - high.astype(jnp.float32)).astype(jnp.bfloat16)


def dot(left, right):
    return jnp.dot(left, right, preferred_element_type=jnp.float32)


def root_kernel(param_ref, packed_ref, out_ref, made_ref, block_ref, high_ref, low_ref, sem):
    count, width = out_ref.shape[0], out_ref.shape[1]
    half = width // 2
    chunks = half // LANE
    full, top, bottom = slice(0, width), slice(0, half), slice(half, width)
    tiles = ((top, top), (bottom, top), (bottom, bottom))
    row_ids = lax.broadcasted_iota(jnp.int32, (half, half), 0)
    col_ids = lax.broadcasted_iota(jnp.int32, (half, half), 1)
    eye = row_ids == col_ids
    slots = range(count)

    def add_eye(values, scalar):
        there = jnp.where(eye, scalar, 0.0)
        return values[0] + there, values[1], values[2] + there

    def store(slot, place, values):
        for tile, value in zip(tiles, values):
            high, low = split(value)
            high_ref[slot, place, tile[0], tile[1]] = high
            low_ref[slot, place, tile[0], tile[1]] = low
            if tile == (bottom, top):
                high_ref[slot, place, top, bottom] = high.T
                low_ref[slot, place, top, bottom] = low.T

    def dots(left, right):
        def some(rows, cols):
            return dot(
                jnp.concatenate([part(rows, full) for part in left], axis=1),
                jnp.concatenate([part(full, cols) for part in right], axis=0),
            )

        lower = some(bottom, full)
        return some(top, top), lower[:, top], lower[:, bottom]

    def at(ref, *place):
        return lambda rows, cols: ref[place + (rows, cols)]

    def product(slot, left, right):
        high, low = at(high_ref, slot, left), at(low_ref, slot, left)
        return dots(
            [high, low, high],
            [at(high_ref, slot, right), at(high_ref, slot, right), at(low_ref, slot, right)],
        )

    def by_block(slot, left):
        block = at(block_ref, slot)
        return dots([at(high_ref, slot, left), at(low_ref, slot, left)], [block, block])

    def block_tiles(slot):
        return [block_ref[slot, rows, cols].astype(jnp.float32) for rows, cols in tiles]

    inverses = [param_ref[slot, chunks:chunks + 1, :1] for slot in slots]
    gains = [param_ref[slot, chunks + 1:chunks + 2, :1] for slot in slots]
    for slot in slots:
        lines = packed_ref[:, slot].reshape(-1, LANE)

        def square(place):
            return jnp.concatenate(
                [lines[(place + c) * half:(place + c + 1) * half] for c in range(chunks)], axis=1
            )

        corner = square(0)
        mixed = square(chunks).astype(jnp.float32)
        turned = mixed.T
        upper = jnp.where(row_ids >= col_ids, mixed, turned)
        lower = jnp.where(row_ids < col_ids, mixed, turned)
        diagonal = jnp.concatenate([param_ref[slot, c:c + 1] for c in range(chunks)], axis=1)
        lower = jnp.where(eye, diagonal, lower)
        block_ref[slot, top, top] = upper.astype(jnp.bfloat16)
        block_ref[slot, bottom, top] = corner
        block_ref[slot, top, bottom] = corner.T
        block_ref[slot, bottom, bottom] = lower.astype(jnp.bfloat16)
    for slot in slots:
        scaled = [(0.25 * inverses[slot]) * tile for tile in block_tiles(slot)]
        squared = dots([at(block_ref, slot)], [at(block_ref, slot)])
        factor = 0.0625 * inverses[slot] * inverses[slot]
        store(
            slot, 0, add_eye([factor * b - 2.5 * a for a, b in zip(scaled, squared)], 1.5625)
        )
    def tile_sum(slot, place):
        return [
            high_ref[slot, place, rows, cols].astype(jnp.float32)
            + low_ref[slot, place, rows, cols].astype(jnp.float32)
            for rows, cols in tiles
        ]

    for slot in slots:
        turned = by_block(slot, 0)
        squares = tile_sum(slot, 0)
        cubes = [1.25 * a - (0.25 * inverses[slot]) * b for a, b in zip(squares, turned)]
        store(slot, 1, cubes)
        store(slot, 2, [a - 1.25 * b for a, b in zip(cubes, squares)])
    for slot in slots:
        sixth = product(slot, 1, 2)
        scaled = [(0.3125 * inverses[slot]) * tile for tile in block_tiles(slot)]
        store(slot, 0, add_eye([b - a for a, b in zip(scaled, sixth)], 1.5625))
    for slot in slots:
        store(slot, 1, product(slot, 0, 0))
    for slot in slots:
        store(slot, 2, product(slot, 1, 1))
    for slot in slots:
        tail = by_block(slot, 2)
        store(slot, 1, add_eye([-(0.25 * inverses[slot]) * tile for tile in tail], 1.25))
    copies = []
    for slot in slots:
        valid = gains[slot] > 0.0
        result = [jnp.where(valid, tile * gains[slot], 0.0) for tile in product(slot, 0, 1)]
        for (rows, cols), tile in zip(tiles, result):
            made_ref[slot, rows, cols] = tile
        made_ref[slot, top, bottom] = result[1].T
        copies.append(pltpu.make_async_copy(made_ref.at[slot], out_ref.at[slot], sem.at[slot]))
        copies[-1].start()
    for copy in copies:
        copy.wait()


def root(params, packed, width):
    count = packed.shape[1]
    return pl.pallas_call(
        root_kernel,
        out_shape=jax.ShapeDtypeStruct((count, width, width), jnp.float32),
        in_specs=[
            pl.BlockSpec(memory_space=pltpu.VMEM),
            pl.BlockSpec(memory_space=pltpu.VMEM),
        ],
        out_specs=pl.BlockSpec(memory_space=pl.ANY),
        scratch_shapes=[
            pltpu.VMEM((count, width, width), jnp.float32),
            pltpu.VMEM((count, width, width), jnp.bfloat16),
            pltpu.VMEM((count, 3, width, width), jnp.bfloat16),
            pltpu.VMEM((count, 3, width, width), jnp.bfloat16),
            pltpu.SemaphoreType.DMA((count,)),
        ],
        cost_estimate=pl.CostEstimate(
            flops=26 * count * width ** 3,
            bytes_accessed=5 * count * width * width,
            transcendentals=0,
        ),
        name="root",
    )(
        pltpu.with_memory_space_constraint(params, pltpu.VMEM),
        pltpu.with_memory_space_constraint(packed, pltpu.VMEM),
    )


def shards(factors, target):
    row_count, col_count = lax.axis_size("row"), lax.axis_size("col")
    hold, width = factors.shape[1], factors.shape[2]
    packed = pack(factors, target, row_count, col_count)
    pieces = lax.all_to_all(packed, RING, split_axis=0, concat_axis=0, tiled=True)
    chosen, params = select(pieces, hold, row_count, col_count, width)
    landed = lax.all_to_all(chosen, RING, split_axis=0, concat_axis=0, tiled=True)
    return root(params, landed, width)[None]


def solution(mesh):
    return jax.shard_map(
        shards,
        mesh=mesh,
        in_specs=(P(AXES, None, None, None), P(AXES, None)),
        out_specs=P(AXES, None, None, None),
        check_vma=False,
    )
```

```python
import functools
import jax
import jax.numpy as jnp
from jax import lax
from jax.experimental import pallas as pl
from jax.experimental.pallas import tpu as pltpu
from jax.sharding import PartitionSpec as P

CAP = 3
LANE = 128
INFO_ROWS = 8
SQUARE_PARTS = 3
NAME_PARTS = 2
LINEAR = -0.625
AXES = ("row", "col")
RING = ("col", "row")


def parts_of(value, count):
    parts = []
    for _ in range(count):
        part = value.astype(jnp.bfloat16)
        parts.append(part)
        value = value - part.astype(jnp.float32)
    return parts


def pack_kernel(row_count, col_count, target_ref, block_ref, packed_ref):
    hold, width = block_ref.shape[1], block_ref.shape[2]
    pieces = packed_ref.shape[0]
    half = width // 2
    depth = (packed_ref.shape[1] - INFO_ROWS) // hold
    row_ids = lax.broadcasted_iota(jnp.int32, (half, half), 0)
    col_ids = lax.broadcasted_iota(jnp.int32, (half, half), 1)
    info = jnp.zeros((INFO_ROWS, LANE), jnp.float32)
    info_row = lax.broadcasted_iota(jnp.int32, (INFO_ROWS, LANE), 0)
    info_col = lax.broadcasted_iota(jnp.int32, (INFO_ROWS, LANE), 1)
    square_sum = jnp.zeros((1, 1), jnp.float32)
    chunks = half // LANE
    for slot in range(hold):
        upper = block_ref[0, slot, :half, :half].astype(jnp.float32)
        corner = block_ref[0, slot, half:, :half]
        lower = block_ref[0, slot, half:, half:].astype(jnp.float32)
        wide = corner.astype(jnp.float32)
        folded = upper * upper + lower * lower + 2.0 * (wide * wide)
        square_sum = square_sum + jnp.sum(jnp.sum(folded, axis=0, keepdims=True), axis=1, keepdims=True)
        diagonal = jnp.sum(jnp.where(row_ids == col_ids, lower, 0.0), axis=0, keepdims=True)
        mixed = jnp.where(row_ids >= col_ids, upper, lower).astype(jnp.bfloat16)
        stripes = [corner[:, c * LANE:(c + 1) * LANE] for c in range(chunks)]
        stripes += [mixed[:, c * LANE:(c + 1) * LANE] for c in range(chunks)]
        per_stripe = half // depth
        for piece in range(pieces):
            stripe, place = piece // per_stripe, piece % per_stripe
            packed_ref[piece, slot * depth:(slot + 1) * depth] = (
                stripes[stripe][place * depth:(place + 1) * depth]
            )
        for c in range(chunks):
            line = diagonal[:, c * LANE:(c + 1) * LANE]
            info = jnp.where(info_row == slot * chunks + c, line, info)
    tail = info_row == hold * chunks
    values = parts_of(square_sum, SQUARE_PARTS)
    for slot in range(hold):
        owner = target_ref[0, slot]
        place = lax.rem(owner, col_count) * row_count + lax.div(owner, col_count)
        place = jnp.zeros((1, 1), jnp.float32) + place.astype(jnp.float32)
        values += parts_of(place, NAME_PARTS)
    for place, value in enumerate(values):
        info = jnp.where(tail & (info_col == place), value.astype(jnp.float32), info)
    info = info.astype(jnp.bfloat16)
    for piece in range(pieces):
        packed_ref[piece, hold * depth:] = info


def pack(factors, target, row_count, col_count):
    hold, width = factors.shape[1], factors.shape[2]
    pieces = row_count * col_count
    depth = width * width // 2 // LANE // pieces
    return pl.pallas_call(
        functools.partial(pack_kernel, row_count, col_count),
        out_shape=pltpu.VMEM((pieces, hold * depth + INFO_ROWS, LANE), jnp.bfloat16),
        in_specs=[
            pl.BlockSpec(memory_space=pltpu.SMEM),
            pl.BlockSpec(memory_space=pltpu.VMEM),
        ],
        out_specs=pl.BlockSpec(memory_space=pltpu.VMEM),
        name="pack",
    )(target.T, factors)


def select_kernel(
    hold, row_count, col_count, width, pieces_ref, chosen_ref, param_ref,
    name_ref, place_ref, count_ref, table_ref, sem,
):
    owners, depth = chosen_ref.shape[0], chosen_ref.shape[2]
    rows = hold * depth
    half_lines = width // 2 // LANE
    info = pieces_ref[:, rows:rows + INFO_ROWS].astype(jnp.float32)
    tail = info[:, hold * half_lines]
    names = [tail]
    for part in range(1, NAME_PARTS):
        names.append(pltpu.roll(tail, LANE - part, 1))
    name_ref[...] = sum(names).astype(jnp.int32)
    copy = pltpu.make_async_copy(name_ref, place_ref, sem)
    copy.start()
    for owner in range(owners):
        count_ref[owner] = 0
    copy.wait()
    for device in range(owners):
        source = (device % col_count) * row_count + device // col_count
        for part in range(hold):
            owner = place_ref[source, SQUARE_PARTS + part * NAME_PARTS]
            slot = count_ref[owner]
            count_ref[owner] = slot + 1
            table_ref[owner, slot] = source * hold + part
            chosen_ref[owner, slot] = pieces_ref[source, part * depth:(part + 1) * depth]
    me = lax.axis_index("col") * row_count + lax.axis_index("row")
    source_ids = lax.broadcasted_iota(jnp.int32, (owners, LANE), 0)
    lanes = lax.broadcasted_iota(jnp.int32, (owners, LANE), 1)
    squares = jnp.where(lanes < SQUARE_PARTS, tail, 0.0)
    for slot in range(CAP):
        valid = slot < count_ref[me]
        code = jnp.where(valid, table_ref[me, slot], 0)
        source, part = lax.div(code, hold), lax.rem(code, hold)
        same_row = lax.rem(source_ids, row_count) == lax.rem(source, row_count)
        total = jnp.sum(
            jnp.sum(jnp.where(same_row, squares, 0.0), axis=0, keepdims=True), axis=1, keepdims=True
        )
        scale = 2.0 * jnp.sqrt(total / (col_count * hold * width))
        inverse = 1.0 / scale
        gain = lax.rsqrt(jnp.sqrt(scale))
        here = pieces_ref[source, rows:rows + INFO_ROWS].astype(jnp.float32)
        diagonal = here[:half_lines]
        for other in range(1, hold):
            lines = here[other * half_lines:(other + 1) * half_lines]
            diagonal = jnp.where(part == other, lines, diagonal)
        param_ref[slot, :half_lines] = diagonal
        one = jnp.zeros((1, LANE), jnp.float32)
        param_ref[slot, half_lines:half_lines + 1] = one + inverse
        param_ref[slot, half_lines + 1:half_lines + 2] = jnp.where(valid, one + gain, 0.0)


def select(pieces, hold, row_count, col_count, width):
    owners = pieces.shape[0]
    depth = (pieces.shape[1] - INFO_ROWS) // hold
    return pl.pallas_call(
        functools.partial(select_kernel, hold, row_count, col_count, width),
        out_shape=(
            pltpu.VMEM((owners, CAP, depth, LANE), pieces.dtype),
            pltpu.VMEM((CAP, INFO_ROWS, LANE), jnp.float32),
        ),
        in_specs=[pl.BlockSpec(memory_space=pltpu.VMEM)],
        out_specs=(
            pl.BlockSpec(memory_space=pltpu.VMEM),
            pl.BlockSpec(memory_space=pltpu.VMEM),
        ),
        scratch_shapes=[
            pltpu.VMEM((owners, LANE), jnp.int32),
            pltpu.SMEM((owners, LANE), jnp.int32),
            pltpu.SMEM((owners,), jnp.int32),
            pltpu.SMEM((owners, CAP), jnp.int32),
            pltpu.SemaphoreType.DMA,
        ],
        name="select",
    )(pltpu.with_memory_space_constraint(pieces, pltpu.VMEM))


def split(value):
    high = value.astype(jnp.bfloat16)
    return high, (value - high.astype(jnp.float32)).astype(jnp.bfloat16)


def dot(left, right):
    return jnp.dot(left, right, preferred_element_type=jnp.float32)


def root_kernel(param_ref, packed_ref, out_ref, made_ref, block_ref, high_ref, low_ref, sem):
    count, width = out_ref.shape[0], out_ref.shape[1]
    half = width // 2
    chunks = half // LANE
    full, top, bottom = slice(0, width), slice(0, half), slice(half, width)
    tiles = ((top, top), (bottom, top), (bottom, bottom))
    row_ids = lax.broadcasted_iota(jnp.int32, (half, half), 0)
    col_ids = lax.broadcasted_iota(jnp.int32, (half, half), 1)
    eye = row_ids == col_ids
    slots = range(count)

    def add_eye(values, scalar):
        there = jnp.where(eye, scalar, 0.0)
        return values[0] + there, values[1], values[2] + there

    def store(slot, place, values):
        for tile, value in zip(tiles, values):
            high, low = split(value)
            high_ref[slot, place, tile[0], tile[1]] = high
            low_ref[slot, place, tile[0], tile[1]] = low
            if tile == (bottom, top):
                high_ref[slot, place, top, bottom] = high.T
                low_ref[slot, place, top, bottom] = low.T

    def dots(left, right):
        def some(rows, cols):
            return dot(
                jnp.concatenate([part(rows, full) for part in left], axis=1),
                jnp.concatenate([part(full, cols) for part in right], axis=0),
            )

        left_half = some(full, top)
        return left_half[top], left_half[bottom], some(bottom, bottom)

    def at(ref, *place):
        return lambda rows, cols: ref[place + (rows, cols)]

    def product(slot, left, right):
        high, low = at(high_ref, slot, left), at(low_ref, slot, left)
        return dots(
            [high, low, high],
            [at(high_ref, slot, right), at(high_ref, slot, right), at(low_ref, slot, right)],
        )

    def square_of(slot, place):
        high, low = at(high_ref, slot, place), at(low_ref, slot, place)
        main = dots([high], [high])
        cross = dot(high(full, full), low(full, full)).astype(jnp.bfloat16)
        flipped = [cross[top, top].T, cross[top, bottom].T, cross[bottom, bottom].T]
        return [
            value + (cross[tile[0], tile[1]].astype(jnp.float32) + other.astype(jnp.float32))
            for value, tile, other in zip(main, tiles, flipped)
        ]

    def by_block(slot, left):
        block = at(block_ref, slot)
        return dots([at(high_ref, slot, left), at(low_ref, slot, left)], [block, block])

    def block_tiles(slot):
        return [block_ref[slot, rows, cols].astype(jnp.float32) for rows, cols in tiles]

    inverses = [param_ref[slot, chunks:chunks + 1, :1] for slot in slots]
    gains = [param_ref[slot, chunks + 1:chunks + 2, :1] for slot in slots]
    for slot in slots:
        lines = packed_ref[:, slot].reshape(-1, LANE)

        def square(place):
            return jnp.concatenate(
                [lines[(place + c) * half:(place + c + 1) * half] for c in range(chunks)], axis=1
            )

        corner = square(0)
        mixed = square(chunks)
        turned = mixed.T.astype(jnp.float32)
        mixed = mixed.astype(jnp.float32)
        upper = jnp.where(row_ids >= col_ids, mixed, turned)
        lower = jnp.where(row_ids < col_ids, mixed, turned)
        diagonal = jnp.concatenate([param_ref[slot, c:c + 1] for c in range(chunks)], axis=1)
        lower = jnp.where(eye, diagonal, lower)
        block_ref[slot, top, top] = upper.astype(jnp.bfloat16)
        block_ref[slot, bottom, top] = corner
        block_ref[slot, top, bottom] = corner.T
        block_ref[slot, bottom, bottom] = lower.astype(jnp.bfloat16)
        scaled = [(0.25 * inverses[slot]) * tile for tile in block_tiles(slot)]
        squared = dots([at(block_ref, slot)], [at(block_ref, slot)])
        factor = 0.0625 * inverses[slot] * inverses[slot]
        store(
            slot, 0, add_eye([factor * b - 2.5 * a for a, b in zip(scaled, squared)], 1.5625)
        )
    def tile_sum(slot, place):
        return [
            high_ref[slot, place, rows, cols].astype(jnp.float32)
            + low_ref[slot, place, rows, cols].astype(jnp.float32)
            for rows, cols in tiles
        ]

    second = -0.5 * LINEAR * LINEAR
    third = -LINEAR * second
    pairs = []
    for slot in slots:
        turned = by_block(slot, 0)
        squares = tile_sum(slot, 0)
        scaled = [(0.25 * inverses[slot]) * tile for tile in block_tiles(slot)]
        near = [
            (1.25 + LINEAR) * b - (0.25 * inverses[slot]) * c - second * a
            for a, b, c in zip(scaled, squares, turned)
        ]
        store(slot, 1, add_eye(near, 1.25 * second + third))
        from_square = second * second + 2.0 * LINEAR * third
        from_step = 2.0 * second * third - 1.25
        rest = [from_step * a - from_square * b for a, b in zip(scaled, squares)]
        pairs.append(add_eye(rest, -1.25 * from_step - third * third))
    for slot in slots:
        store(slot, 0, [a + b for a, b in zip(square_of(slot, 1), pairs[slot])])
    for slot in slots:
        store(slot, 1, square_of(slot, 0))
    for slot in slots:
        store(slot, 2, square_of(slot, 1))
    for slot in slots:
        tail = by_block(slot, 2)
        store(slot, 1, add_eye([-(0.25 * inverses[slot]) * tile for tile in tail], 1.25))
    copies = []
    for slot in slots:
        valid = gains[slot] > 0.0
        result = [jnp.where(valid, tile * gains[slot], 0.0) for tile in product(slot, 0, 1)]
        for place, rows in enumerate((bottom, top)):
            if rows == bottom:
                made_ref[slot, bottom, top] = result[1]
                made_ref[slot, bottom, bottom] = result[2]
            else:
                made_ref[slot, top, top] = result[0]
                made_ref[slot, top, bottom] = result[1].T
            span = pl.ds(rows.start, half)
            copies.append(
                pltpu.make_async_copy(
                    made_ref.at[slot, span], out_ref.at[slot, span], sem.at[slot, place]
                )
            )
            copies[-1].start()
    for copy in copies:
        copy.wait()


def root(params, packed, width):
    count = packed.shape[1]
    return pl.pallas_call(
        root_kernel,
        out_shape=jax.ShapeDtypeStruct((count, width, width), jnp.float32),
        in_specs=[
            pl.BlockSpec(memory_space=pltpu.VMEM),
            pl.BlockSpec(memory_space=pltpu.VMEM),
        ],
        out_specs=pl.BlockSpec(memory_space=pl.ANY),
        scratch_shapes=[
            pltpu.VMEM((count, width, width), jnp.float32),
            pltpu.VMEM((count, width, width), jnp.bfloat16),
            pltpu.VMEM((count, 3, width, width), jnp.bfloat16),
            pltpu.VMEM((count, 3, width, width), jnp.bfloat16),
            pltpu.SemaphoreType.DMA((count, 2)),
        ],
        cost_estimate=pl.CostEstimate(
            flops=26 * count * width ** 3,
            bytes_accessed=5 * count * width * width,
            transcendentals=0,
        ),
        name="root",
    )(
        pltpu.with_memory_space_constraint(params, pltpu.VMEM),
        pltpu.with_memory_space_constraint(packed, pltpu.VMEM),
    )


def shards(factors, target):
    row_count, col_count = lax.axis_size("row"), lax.axis_size("col")
    hold, width = factors.shape[1], factors.shape[2]
    packed = pack(factors, target, row_count, col_count)
    pieces = lax.all_to_all(packed, RING, split_axis=0, concat_axis=0, tiled=True)
    chosen, params = select(pieces, hold, row_count, col_count, width)
    landed = lax.all_to_all(chosen, RING, split_axis=0, concat_axis=0, tiled=True)
    return root(params, landed, width)[None]


def solution(mesh):
    return jax.shard_map(
        shards,
        mesh=mesh,
        in_specs=(P(AXES, None, None, None), P(AXES, None)),
        out_specs=P(AXES, None, None, None),
        check_vma=False,
    )
```

```python
import functools
import jax
import jax.numpy as jnp
from jax import lax
from jax.experimental import pallas as pl
from jax.experimental.pallas import tpu as pltpu
from jax.sharding import PartitionSpec as P

CAP = 3
LANE = 128
INFO_ROWS = 8
SQUARE_PARTS = 3
NAME_PARTS = 2
LINEAR = -0.625
AXES = ("row", "col")
RING = ("col", "row")


def parts_of(value, count):
    parts = []
    for _ in range(count):
        part = value.astype(jnp.bfloat16)
        parts.append(part)
        value = value - part.astype(jnp.float32)
    return parts


def pack_kernel(row_count, col_count, target_ref, block_ref, packed_ref):
    hold, width = block_ref.shape[1], block_ref.shape[2]
    pieces = packed_ref.shape[0]
    half = width // 2
    depth = (packed_ref.shape[1] - INFO_ROWS) // hold
    row_ids = lax.broadcasted_iota(jnp.int32, (half, half), 0)
    col_ids = lax.broadcasted_iota(jnp.int32, (half, half), 1)
    info = jnp.zeros((INFO_ROWS, LANE), jnp.float32)
    info_row = lax.broadcasted_iota(jnp.int32, (INFO_ROWS, LANE), 0)
    info_col = lax.broadcasted_iota(jnp.int32, (INFO_ROWS, LANE), 1)
    square_sum = jnp.zeros((1, 1), jnp.float32)
    chunks = half // LANE
    for slot in range(hold):
        upper = block_ref[0, slot, :half, :half].astype(jnp.float32)
        corner = block_ref[0, slot, half:, :half]
        lower = block_ref[0, slot, half:, half:].astype(jnp.float32)
        wide = corner.astype(jnp.float32)
        folded = upper * upper + lower * lower + 2.0 * (wide * wide)
        square_sum = square_sum + jnp.sum(jnp.sum(folded, axis=0, keepdims=True), axis=1, keepdims=True)
        diagonal = jnp.sum(jnp.where(row_ids == col_ids, lower, 0.0), axis=0, keepdims=True)
        mixed = jnp.where(row_ids >= col_ids, upper, lower).astype(jnp.bfloat16)
        stripes = [corner[:, c * LANE:(c + 1) * LANE] for c in range(chunks)]
        stripes += [mixed[:, c * LANE:(c + 1) * LANE] for c in range(chunks)]
        per_stripe = half // depth
        for piece in range(pieces):
            stripe, place = piece // per_stripe, piece % per_stripe
            packed_ref[piece, slot * depth:(slot + 1) * depth] = (
                stripes[stripe][place * depth:(place + 1) * depth]
            )
        for c in range(chunks):
            line = diagonal[:, c * LANE:(c + 1) * LANE]
            info = jnp.where(info_row == slot * chunks + c, line, info)
    tail = info_row == hold * chunks
    values = parts_of(square_sum, SQUARE_PARTS)
    for slot in range(hold):
        owner = target_ref[0, slot]
        place = lax.rem(owner, col_count) * row_count + lax.div(owner, col_count)
        place = jnp.zeros((1, 1), jnp.float32) + place.astype(jnp.float32)
        values += parts_of(place, NAME_PARTS)
    for place, value in enumerate(values):
        info = jnp.where(tail & (info_col == place), value.astype(jnp.float32), info)
    info = info.astype(jnp.bfloat16)
    for piece in range(pieces):
        packed_ref[piece, hold * depth:] = info


def pack(factors, target, row_count, col_count):
    hold, width = factors.shape[1], factors.shape[2]
    pieces = row_count * col_count
    depth = width * width // 2 // LANE // pieces
    return pl.pallas_call(
        functools.partial(pack_kernel, row_count, col_count),
        out_shape=pltpu.VMEM((pieces, hold * depth + INFO_ROWS, LANE), jnp.bfloat16),
        in_specs=[
            pl.BlockSpec(memory_space=pltpu.SMEM),
            pl.BlockSpec(memory_space=pltpu.VMEM),
        ],
        out_specs=pl.BlockSpec(memory_space=pltpu.VMEM),
        name="pack",
    )(target.T, factors)


def select_kernel(
    hold, row_count, col_count, width, pieces_ref, chosen_ref, param_ref,
    count_ref, table_ref,
):
    owners, depth = chosen_ref.shape[0], chosen_ref.shape[2]
    rows = hold * depth
    half_lines = width // 2 // LANE
    info = pieces_ref[:, rows:rows + INFO_ROWS].astype(jnp.float32)
    tail = info[:, hold * half_lines]
    names = [tail]
    for part in range(1, NAME_PARTS):
        names.append(pltpu.roll(tail, LANE - part, 1))
    places = sum(names).astype(jnp.int32)
    for owner in range(owners):
        count_ref[owner] = 0
    for device in range(owners):
        source = (device % col_count) * row_count + device // col_count
        for part in range(hold):
            owner = places[source, SQUARE_PARTS + part * NAME_PARTS]
            slot = count_ref[owner]
            count_ref[owner] = slot + 1
            table_ref[owner, slot] = source * hold + part
            chosen_ref[owner, slot] = pieces_ref[source, part * depth:(part + 1) * depth]
    me = lax.axis_index("col") * row_count + lax.axis_index("row")
    source_ids = lax.broadcasted_iota(jnp.int32, (owners, LANE), 0)
    lanes = lax.broadcasted_iota(jnp.int32, (owners, LANE), 1)
    squares = jnp.where(lanes < SQUARE_PARTS, tail, 0.0)
    for slot in range(CAP):
        valid = slot < count_ref[me]
        code = jnp.where(valid, table_ref[me, slot], 0)
        source, part = lax.div(code, hold), lax.rem(code, hold)
        same_row = lax.rem(source_ids, row_count) == lax.rem(source, row_count)
        total = jnp.sum(
            jnp.sum(jnp.where(same_row, squares, 0.0), axis=0, keepdims=True), axis=1, keepdims=True
        )
        scale = 2.0 * jnp.sqrt(total / (col_count * hold * width))
        inverse = 1.0 / scale
        gain = lax.rsqrt(jnp.sqrt(scale))
        here = pieces_ref[source, rows:rows + INFO_ROWS].astype(jnp.float32)
        diagonal = here[:half_lines]
        for other in range(1, hold):
            lines = here[other * half_lines:(other + 1) * half_lines]
            diagonal = jnp.where(part == other, lines, diagonal)
        param_ref[slot, :half_lines] = diagonal
        one = jnp.zeros((1, LANE), jnp.float32)
        param_ref[slot, half_lines:half_lines + 1] = one + inverse
        param_ref[slot, half_lines + 1:half_lines + 2] = jnp.where(valid, one + gain, 0.0)


def select(pieces, hold, row_count, col_count, width):
    owners = pieces.shape[0]
    depth = (pieces.shape[1] - INFO_ROWS) // hold
    return pl.pallas_call(
        functools.partial(select_kernel, hold, row_count, col_count, width),
        out_shape=(
            pltpu.VMEM((owners, CAP, depth, LANE), pieces.dtype),
            pltpu.VMEM((CAP, INFO_ROWS, LANE), jnp.float32),
        ),
        in_specs=[pl.BlockSpec(memory_space=pltpu.VMEM)],
        out_specs=(
            pl.BlockSpec(memory_space=pltpu.VMEM),
            pl.BlockSpec(memory_space=pltpu.VMEM),
        ),
        scratch_shapes=[
            pltpu.SMEM((owners,), jnp.int32),
            pltpu.SMEM((owners, CAP), jnp.int32),
        ],
        name="select",
    )(pltpu.with_memory_space_constraint(pieces, pltpu.VMEM))


def split(value):
    high = value.astype(jnp.bfloat16)
    return high, (value - high.astype(jnp.float32)).astype(jnp.bfloat16)


def dot(left, right):
    return jnp.dot(left, right, preferred_element_type=jnp.float32)


def root_kernel(param_ref, packed_ref, out_ref, made_ref, block_ref, high_ref, low_ref, sem):
    count, width = out_ref.shape[0], out_ref.shape[1]
    half = width // 2
    chunks = half // LANE
    full, top, bottom = slice(0, width), slice(0, half), slice(half, width)
    tiles = ((top, top), (bottom, top), (bottom, bottom))
    row_ids = lax.broadcasted_iota(jnp.int32, (half, half), 0)
    col_ids = lax.broadcasted_iota(jnp.int32, (half, half), 1)
    eye = row_ids == col_ids
    slots = range(count)

    def add_eye(values, scalar):
        there = jnp.where(eye, scalar, 0.0)
        return values[0] + there, values[1], values[2] + there

    def store(slot, place, values):
        for tile, value in zip(tiles, values):
            high, low = split(value)
            high_ref[slot, place, tile[0], tile[1]] = high
            low_ref[slot, place, tile[0], tile[1]] = low
            if tile == (bottom, top):
                high_ref[slot, place, top, bottom] = high.T
                low_ref[slot, place, top, bottom] = low.T

    def dots(left, right):
        def some(rows, cols):
            return dot(
                jnp.concatenate([part(rows, full) for part in left], axis=1),
                jnp.concatenate([part(full, cols) for part in right], axis=0),
            )

        left_half = some(full, top)
        return left_half[top], left_half[bottom], some(bottom, bottom)

    def at(ref, *place):
        return lambda rows, cols: ref[place + (rows, cols)]

    def product(slot, left, right):
        high, low = at(high_ref, slot, left), at(low_ref, slot, left)
        return dots(
            [high, low, high],
            [at(high_ref, slot, right), at(high_ref, slot, right), at(low_ref, slot, right)],
        )

    def square_of(slot, place):
        high, low = at(high_ref, slot, place), at(low_ref, slot, place)
        main = dots([high], [high])
        cross = dot(high(full, full), low(full, full)).astype(jnp.bfloat16)
        flipped = [cross[top, top].T, cross[top, bottom].T, cross[bottom, bottom].T]
        return [
            value + (cross[tile[0], tile[1]].astype(jnp.float32) + other.astype(jnp.float32))
            for value, tile, other in zip(main, tiles, flipped)
        ]

    def by_block(slot, left):
        block = at(block_ref, slot)
        return dots([at(high_ref, slot, left), at(low_ref, slot, left)], [block, block])

    def block_tiles(slot):
        return [block_ref[slot, rows, cols].astype(jnp.float32) for rows, cols in tiles]

    inverses = [param_ref[slot, chunks:chunks + 1, :1] for slot in slots]
    gains = [param_ref[slot, chunks + 1:chunks + 2, :1] for slot in slots]
    for slot in slots:
        lines = packed_ref[:, slot].reshape(-1, LANE)

        def square(place):
            return jnp.concatenate(
                [lines[(place + c) * half:(place + c + 1) * half] for c in range(chunks)], axis=1
            )

        corner = square(0)
        mixed = square(chunks)
        turned = mixed.T.astype(jnp.float32)
        mixed = mixed.astype(jnp.float32)
        upper = jnp.where(row_ids >= col_ids, mixed, turned)
        lower = jnp.where(row_ids < col_ids, mixed, turned)
        diagonal = jnp.concatenate([param_ref[slot, c:c + 1] for c in range(chunks)], axis=1)
        lower = jnp.where(eye, diagonal, lower)
        block_ref[slot, top, top] = upper.astype(jnp.bfloat16)
        block_ref[slot, bottom, top] = corner
        block_ref[slot, top, bottom] = corner.T
        block_ref[slot, bottom, bottom] = lower.astype(jnp.bfloat16)
        scaled = [(0.25 * inverses[slot]) * tile for tile in block_tiles(slot)]
        squared = dots([at(block_ref, slot)], [at(block_ref, slot)])
        factor = 0.0625 * inverses[slot] * inverses[slot]
        store(
            slot, 0, add_eye([factor * b - 2.5 * a for a, b in zip(scaled, squared)], 1.5625)
        )
    def tile_sum(slot, place):
        return [
            high_ref[slot, place, rows, cols].astype(jnp.float32)
            + low_ref[slot, place, rows, cols].astype(jnp.float32)
            for rows, cols in tiles
        ]

    second = -0.5 * LINEAR * LINEAR
    third = -LINEAR * second
    pairs = []
    for slot in slots:
        turned = by_block(slot, 0)
        squares = tile_sum(slot, 0)
        scaled = [(0.25 * inverses[slot]) * tile for tile in block_tiles(slot)]
        near = [
            (1.25 + LINEAR) * b - (0.25 * inverses[slot]) * c - second * a
            for a, b, c in zip(scaled, squares, turned)
        ]
        store(slot, 1, add_eye(near, 1.25 * second + third))
        from_square = second * second + 2.0 * LINEAR * third
        from_step = 2.0 * second * third - 1.25
        rest = [from_step * a - from_square * b for a, b in zip(scaled, squares)]
        pairs.append(add_eye(rest, -1.25 * from_step - third * third))
    for slot in slots:
        store(slot, 0, [a + b for a, b in zip(square_of(slot, 1), pairs[slot])])
    for slot in slots:
        store(slot, 1, square_of(slot, 0))
    for slot in slots:
        store(slot, 2, square_of(slot, 1))
    for slot in slots:
        tail = by_block(slot, 2)
        store(slot, 1, add_eye([-(0.25 * inverses[slot]) * tile for tile in tail], 1.25))
    copies = []
    for slot in slots:
        valid = gains[slot] > 0.0
        result = [jnp.where(valid, tile * gains[slot], 0.0) for tile in product(slot, 0, 1)]
        for place, rows in enumerate((bottom, top)):
            if rows == bottom:
                made_ref[slot, bottom, top] = result[1]
                made_ref[slot, bottom, bottom] = result[2]
            else:
                made_ref[slot, top, top] = result[0]
                made_ref[slot, top, bottom] = result[1].T
            span = pl.ds(rows.start, half)
            copies.append(
                pltpu.make_async_copy(
                    made_ref.at[slot, span], out_ref.at[slot, span], sem.at[slot, place]
                )
            )
            copies[-1].start()
    for copy in copies:
        copy.wait()


def root(params, packed, width):
    count = packed.shape[1]
    return pl.pallas_call(
        root_kernel,
        out_shape=jax.ShapeDtypeStruct((count, width, width), jnp.float32),
        in_specs=[
            pl.BlockSpec(memory_space=pltpu.VMEM),
            pl.BlockSpec(memory_space=pltpu.VMEM),
        ],
        out_specs=pl.BlockSpec(memory_space=pl.ANY),
        scratch_shapes=[
            pltpu.VMEM((count, width, width), jnp.float32),
            pltpu.VMEM((count, width, width), jnp.bfloat16),
            pltpu.VMEM((count, 3, width, width), jnp.bfloat16),
            pltpu.VMEM((count, 3, width, width), jnp.bfloat16),
            pltpu.SemaphoreType.DMA((count, 2)),
        ],
        cost_estimate=pl.CostEstimate(
            flops=26 * count * width ** 3,
            bytes_accessed=5 * count * width * width,
            transcendentals=0,
        ),
        name="root",
    )(
        pltpu.with_memory_space_constraint(params, pltpu.VMEM),
        pltpu.with_memory_space_constraint(packed, pltpu.VMEM),
    )


def shards(factors, target):
    row_count, col_count = lax.axis_size("row"), lax.axis_size("col")
    hold, width = factors.shape[1], factors.shape[2]
    packed = pack(factors, target, row_count, col_count)
    pieces = lax.all_to_all(packed, RING, split_axis=0, concat_axis=0, tiled=True)
    chosen, params = select(pieces, hold, row_count, col_count, width)
    landed = lax.all_to_all(chosen, RING, split_axis=0, concat_axis=0, tiled=True)
    return root(params, landed, width)[None]


def solution(mesh):
    return jax.shard_map(
        shards,
        mesh=mesh,
        in_specs=(P(AXES, None, None, None), P(AXES, None)),
        out_specs=P(AXES, None, None, None),
        check_vma=False,
    )
```

```python
import functools
import jax
import jax.numpy as jnp
from jax import lax
from jax.experimental import pallas as pl
from jax.experimental.pallas import tpu as pltpu
from jax.sharding import PartitionSpec as P

CAP = 3
LANE = 128
INFO_ROWS = 8
SQUARE_PARTS = 3
NAME_PARTS = 2
LINEAR = -0.625
AXES = ("row", "col")
RING = ("col", "row")


def parts_of(value, count):
    parts = []
    for _ in range(count):
        part = value.astype(jnp.bfloat16)
        parts.append(part)
        value = value - part.astype(jnp.float32)
    return parts


def pack_kernel(row_count, col_count, target_ref, *refs):
    packed_ref, block_refs = refs[-1], refs[:-1]
    hold, width = len(block_refs) // 2, block_refs[0].shape[2]
    pieces = packed_ref.shape[0]
    half = width // 2
    depth = (packed_ref.shape[1] - INFO_ROWS) // hold
    row_ids = lax.broadcasted_iota(jnp.int32, (half, half), 0)
    col_ids = lax.broadcasted_iota(jnp.int32, (half, half), 1)
    info = jnp.zeros((INFO_ROWS, LANE), jnp.float32)
    info_row = lax.broadcasted_iota(jnp.int32, (INFO_ROWS, LANE), 0)
    info_col = lax.broadcasted_iota(jnp.int32, (INFO_ROWS, LANE), 1)
    square_sum = jnp.zeros((1, 1), jnp.float32)
    chunks = half // LANE
    for slot in range(hold):
        left_ref, lower_ref = block_refs[2 * slot:2 * slot + 2]
        upper = left_ref[0, 0, :half].astype(jnp.float32)
        corner = left_ref[0, 0, half:]
        lower = lower_ref[0, 0].astype(jnp.float32)
        wide = corner.astype(jnp.float32)
        folded = upper * upper + lower * lower + 2.0 * (wide * wide)
        square_sum = square_sum + jnp.sum(jnp.sum(folded, axis=0, keepdims=True), axis=1, keepdims=True)
        diagonal = jnp.sum(jnp.where(row_ids == col_ids, lower, 0.0), axis=0, keepdims=True)
        mixed = jnp.where(row_ids >= col_ids, upper, lower).astype(jnp.bfloat16)
        stripes = [corner[:, c * LANE:(c + 1) * LANE] for c in range(chunks)]
        stripes += [mixed[:, c * LANE:(c + 1) * LANE] for c in range(chunks)]
        per_stripe = half // depth
        for piece in range(pieces):
            stripe, place = piece // per_stripe, piece % per_stripe
            packed_ref[piece, slot * depth:(slot + 1) * depth] = (
                stripes[stripe][place * depth:(place + 1) * depth]
            )
        for c in range(chunks):
            line = diagonal[:, c * LANE:(c + 1) * LANE]
            info = jnp.where(info_row == slot * chunks + c, line, info)
    tail = info_row == hold * chunks
    values = parts_of(square_sum, SQUARE_PARTS)
    for slot in range(hold):
        owner = target_ref[0, slot]
        place = lax.rem(owner, col_count) * row_count + lax.div(owner, col_count)
        place = jnp.zeros((1, 1), jnp.float32) + place.astype(jnp.float32)
        values += parts_of(place, NAME_PARTS)
    for place, value in enumerate(values):
        info = jnp.where(tail & (info_col == place), value.astype(jnp.float32), info)
    info = info.astype(jnp.bfloat16)
    for piece in range(pieces):
        packed_ref[piece, hold * depth:] = info


def pack(factors, target, row_count, col_count):
    hold, width = factors.shape[1], factors.shape[2]
    pieces = row_count * col_count
    depth = width * width // 2 // LANE // pieces
    half = width // 2
    in_specs = [pl.BlockSpec(memory_space=pltpu.SMEM)]
    for slot in range(hold):
        in_specs.append(pl.BlockSpec((1, 1, width, half), lambda i, slot=slot: (0, slot, 0, 0)))
        in_specs.append(pl.BlockSpec((1, 1, half, half), lambda i, slot=slot: (0, slot, 1, 1)))
    return pl.pallas_call(
        functools.partial(pack_kernel, row_count, col_count),
        out_shape=pltpu.VMEM((pieces, hold * depth + INFO_ROWS, LANE), jnp.bfloat16),
        grid=(1,),
        in_specs=in_specs,
        out_specs=pl.BlockSpec(memory_space=pltpu.VMEM),
        name="pack",
    )(target.T, *([factors] * (2 * hold)))


def select_kernel(
    hold, row_count, col_count, width, pieces_ref, chosen_ref, param_ref,
    count_ref, table_ref,
):
    owners, depth = chosen_ref.shape[0], chosen_ref.shape[2]
    rows = hold * depth
    half_lines = width // 2 // LANE
    info = pieces_ref[:, rows:rows + INFO_ROWS].astype(jnp.float32)
    tail = info[:, hold * half_lines]
    names = [tail]
    for part in range(1, NAME_PARTS):
        names.append(pltpu.roll(tail, LANE - part, 1))
    places = sum(names).astype(jnp.int32)
    for owner in range(owners):
        count_ref[owner] = 0
    for device in range(owners):
        source = (device % col_count) * row_count + device // col_count
        for part in range(hold):
            owner = places[source, SQUARE_PARTS + part * NAME_PARTS]
            slot = count_ref[owner]
            count_ref[owner] = slot + 1
            table_ref[owner, slot] = source * hold + part
            chosen_ref[owner, slot] = pieces_ref[source, part * depth:(part + 1) * depth]
    me = lax.axis_index("col") * row_count + lax.axis_index("row")
    source_ids = lax.broadcasted_iota(jnp.int32, (owners, LANE), 0)
    lanes = lax.broadcasted_iota(jnp.int32, (owners, LANE), 1)
    squares = jnp.where(lanes < SQUARE_PARTS, tail, 0.0)
    for slot in range(CAP):
        valid = slot < count_ref[me]
        code = jnp.where(valid, table_ref[me, slot], 0)
        source, part = lax.div(code, hold), lax.rem(code, hold)
        same_row = lax.rem(source_ids, row_count) == lax.rem(source, row_count)
        total = jnp.sum(
            jnp.sum(jnp.where(same_row, squares, 0.0), axis=0, keepdims=True), axis=1, keepdims=True
        )
        scale = 2.0 * jnp.sqrt(total / (col_count * hold * width))
        inverse = 1.0 / scale
        gain = lax.rsqrt(jnp.sqrt(scale))
        here = pieces_ref[source, rows:rows + INFO_ROWS].astype(jnp.float32)
        diagonal = here[:half_lines]
        for other in range(1, hold):
            lines = here[other * half_lines:(other + 1) * half_lines]
            diagonal = jnp.where(part == other, lines, diagonal)
        param_ref[slot, :half_lines] = diagonal
        one = jnp.zeros((1, LANE), jnp.float32)
        param_ref[slot, half_lines:half_lines + 1] = one + inverse
        param_ref[slot, half_lines + 1:half_lines + 2] = jnp.where(valid, one + gain, 0.0)


def select(pieces, hold, row_count, col_count, width):
    owners = pieces.shape[0]
    depth = (pieces.shape[1] - INFO_ROWS) // hold
    return pl.pallas_call(
        functools.partial(select_kernel, hold, row_count, col_count, width),
        out_shape=(
            pltpu.VMEM((owners, CAP, depth, LANE), pieces.dtype),
            pltpu.VMEM((CAP, INFO_ROWS, LANE), jnp.float32),
        ),
        in_specs=[pl.BlockSpec(memory_space=pltpu.VMEM)],
        out_specs=(
            pl.BlockSpec(memory_space=pltpu.VMEM),
            pl.BlockSpec(memory_space=pltpu.VMEM),
        ),
        scratch_shapes=[
            pltpu.SMEM((owners,), jnp.int32),
            pltpu.SMEM((owners, CAP), jnp.int32),
        ],
        name="select",
    )(pltpu.with_memory_space_constraint(pieces, pltpu.VMEM))


def split(value):
    high = value.astype(jnp.bfloat16)
    return high, (value - high.astype(jnp.float32)).astype(jnp.bfloat16)


def dot(left, right):
    return jnp.dot(left, right, preferred_element_type=jnp.float32)


def root_kernel(param_ref, packed_ref, out_ref, made_ref, block_ref, high_ref, low_ref, sem):
    count, width = out_ref.shape[0], out_ref.shape[1]
    half = width // 2
    chunks = half // LANE
    full, top, bottom = slice(0, width), slice(0, half), slice(half, width)
    tiles = ((top, top), (bottom, top), (bottom, bottom))
    row_ids = lax.broadcasted_iota(jnp.int32, (half, half), 0)
    col_ids = lax.broadcasted_iota(jnp.int32, (half, half), 1)
    eye = row_ids == col_ids
    slots = range(count)

    def add_eye(values, scalar):
        there = jnp.where(eye, scalar, 0.0)
        return values[0] + there, values[1], values[2] + there

    def store(slot, place, values):
        for tile, value in zip(tiles, values):
            high, low = split(value)
            high_ref[slot, place, tile[0], tile[1]] = high
            low_ref[slot, place, tile[0], tile[1]] = low
            if tile == (bottom, top):
                high_ref[slot, place, top, bottom] = high.T
                low_ref[slot, place, top, bottom] = low.T

    def dots(left, right):
        def some(rows, cols):
            return dot(
                jnp.concatenate([part(rows, full) for part in left], axis=1),
                jnp.concatenate([part(full, cols) for part in right], axis=0),
            )

        left_half = some(full, top)
        return left_half[top], left_half[bottom], some(bottom, bottom)

    def at(ref, *place):
        return lambda rows, cols: ref[place + (rows, cols)]

    def product(slot, left, right):
        high, low = at(high_ref, slot, left), at(low_ref, slot, left)
        return dots(
            [high, low, high],
            [at(high_ref, slot, right), at(high_ref, slot, right), at(low_ref, slot, right)],
        )

    def square_of(slot, place):
        high, low = at(high_ref, slot, place), at(low_ref, slot, place)
        main = dots([high], [high])
        cross = dot(high(full, full), low(full, full)).astype(jnp.bfloat16)
        flipped = [cross[top, top].T, cross[top, bottom].T, cross[bottom, bottom].T]
        return [
            value + (cross[tile[0], tile[1]].astype(jnp.float32) + other.astype(jnp.float32))
            for value, tile, other in zip(main, tiles, flipped)
        ]

    def by_block(slot, left):
        block = at(block_ref, slot)
        return dots([at(high_ref, slot, left), at(low_ref, slot, left)], [block, block])

    def block_tiles(slot):
        return [block_ref[slot, rows, cols].astype(jnp.float32) for rows, cols in tiles]

    inverses = [param_ref[slot, chunks:chunks + 1, :1] for slot in slots]
    gains = [param_ref[slot, chunks + 1:chunks + 2, :1] for slot in slots]
    for slot in slots:
        lines = packed_ref[:, slot].reshape(-1, LANE)

        def square(place):
            return jnp.concatenate(
                [lines[(place + c) * half:(place + c + 1) * half] for c in range(chunks)], axis=1
            )

        corner = square(0)
        mixed = square(chunks)
        turned = mixed.T.astype(jnp.float32)
        mixed = mixed.astype(jnp.float32)
        upper = jnp.where(row_ids >= col_ids, mixed, turned)
        lower = jnp.where(row_ids < col_ids, mixed, turned)
        diagonal = jnp.concatenate([param_ref[slot, c:c + 1] for c in range(chunks)], axis=1)
        lower = jnp.where(eye, diagonal, lower)
        block_ref[slot, top, top] = upper.astype(jnp.bfloat16)
        block_ref[slot, bottom, top] = corner
        block_ref[slot, top, bottom] = corner.T
        block_ref[slot, bottom, bottom] = lower.astype(jnp.bfloat16)
        scaled = [(0.25 * inverses[slot]) * tile for tile in block_tiles(slot)]
        squared = dots([at(block_ref, slot)], [at(block_ref, slot)])
        factor = 0.0625 * inverses[slot] * inverses[slot]
        store(
            slot, 0, add_eye([factor * b - 2.5 * a for a, b in zip(scaled, squared)], 1.5625)
        )
    def tile_sum(slot, place):
        return [
            high_ref[slot, place, rows, cols].astype(jnp.float32)
            + low_ref[slot, place, rows, cols].astype(jnp.float32)
            for rows, cols in tiles
        ]

    second = -0.5 * LINEAR * LINEAR
    third = -LINEAR * second
    pairs = []
    for slot in slots:
        turned = by_block(slot, 0)
        squares = tile_sum(slot, 0)
        scaled = [(0.25 * inverses[slot]) * tile for tile in block_tiles(slot)]
        near = [
            (1.25 + LINEAR) * b - (0.25 * inverses[slot]) * c - second * a
            for a, b, c in zip(scaled, squares, turned)
        ]
        store(slot, 1, add_eye(near, 1.25 * second + third))
        from_square = second * second + 2.0 * LINEAR * third
        from_step = 2.0 * second * third - 1.25
        rest = [from_step * a - from_square * b for a, b in zip(scaled, squares)]
        pairs.append(add_eye(rest, -1.25 * from_step - third * third))
    for slot in slots:
        store(slot, 0, [a + b for a, b in zip(square_of(slot, 1), pairs[slot])])
    for slot in slots:
        store(slot, 1, square_of(slot, 0))
    for slot in slots:
        store(slot, 2, square_of(slot, 1))
    for slot in slots:
        tail = by_block(slot, 2)
        store(slot, 1, add_eye([-(0.25 * inverses[slot]) * tile for tile in tail], 1.25))
    copies = []
    for slot in slots:
        valid = gains[slot] > 0.0
        result = [jnp.where(valid, tile * gains[slot], 0.0) for tile in product(slot, 0, 1)]
        for place, rows in enumerate((bottom, top)):
            if rows == bottom:
                made_ref[slot, bottom, top] = result[1]
                made_ref[slot, bottom, bottom] = result[2]
            else:
                made_ref[slot, top, top] = result[0]
                made_ref[slot, top, bottom] = result[1].T
            span = pl.ds(rows.start, half)
            copies.append(
                pltpu.make_async_copy(
                    made_ref.at[slot, span], out_ref.at[slot, span], sem.at[slot, place]
                )
            )
            copies[-1].start()
    for copy in copies:
        copy.wait()


def root(params, packed, width):
    count = packed.shape[1]
    return pl.pallas_call(
        root_kernel,
        out_shape=jax.ShapeDtypeStruct((count, width, width), jnp.float32),
        in_specs=[
            pl.BlockSpec(memory_space=pltpu.VMEM),
            pl.BlockSpec(memory_space=pltpu.VMEM),
        ],
        out_specs=pl.BlockSpec(memory_space=pl.ANY),
        scratch_shapes=[
            pltpu.VMEM((count, width, width), jnp.float32),
            pltpu.VMEM((count, width, width), jnp.bfloat16),
            pltpu.VMEM((count, 3, width, width), jnp.bfloat16),
            pltpu.VMEM((count, 3, width, width), jnp.bfloat16),
            pltpu.SemaphoreType.DMA((count, 2)),
        ],
        cost_estimate=pl.CostEstimate(
            flops=26 * count * width ** 3,
            bytes_accessed=5 * count * width * width,
            transcendentals=0,
        ),
        name="root",
    )(
        pltpu.with_memory_space_constraint(params, pltpu.VMEM),
        pltpu.with_memory_space_constraint(packed, pltpu.VMEM),
    )


def shards(factors, target):
    row_count, col_count = lax.axis_size("row"), lax.axis_size("col")
    hold, width = factors.shape[1], factors.shape[2]
    packed = pack(factors, target, row_count, col_count)
    pieces = lax.all_to_all(packed, RING, split_axis=0, concat_axis=0, tiled=True)
    chosen, params = select(pieces, hold, row_count, col_count, width)
    landed = lax.all_to_all(chosen, RING, split_axis=0, concat_axis=0, tiled=True)
    return root(params, landed, width)[None]


def solution(mesh):
    return jax.shard_map(
        shards,
        mesh=mesh,
        in_specs=(P(AXES, None, None, None), P(AXES, None)),
        out_specs=P(AXES, None, None, None),
        check_vma=False,
    )
```

```python
import functools
import jax
import jax.numpy as jnp
from jax import lax
from jax.experimental import pallas as pl
from jax.experimental.pallas import tpu as pltpu
from jax.sharding import PartitionSpec as P

CAP = 3
LANE = 128
INFO_ROWS = 8
SQUARE_PARTS = 3
NAME_PARTS = 2
LINEAR = -0.625
AXES = ("row", "col")
RING = ("col", "row")


def parts_of(value, count):
    parts = []
    for _ in range(count):
        part = value.astype(jnp.bfloat16)
        parts.append(part)
        value = value - part.astype(jnp.float32)
    return parts


def pack_kernel(row_count, col_count, target_ref, *refs):
    packed_ref, block_refs = refs[-1], refs[:-1]
    hold, width = len(block_refs) // 2, block_refs[0].shape[2]
    pieces = packed_ref.shape[0]
    half = width // 2
    depth = (packed_ref.shape[1] - INFO_ROWS) // hold
    row_ids = lax.broadcasted_iota(jnp.int32, (half, half), 0)
    col_ids = lax.broadcasted_iota(jnp.int32, (half, half), 1)
    info = jnp.zeros((INFO_ROWS, LANE), jnp.float32)
    info_row = lax.broadcasted_iota(jnp.int32, (INFO_ROWS, LANE), 0)
    info_col = lax.broadcasted_iota(jnp.int32, (INFO_ROWS, LANE), 1)
    square_sum = jnp.zeros((1, 1), jnp.float32)
    chunks = half // LANE
    for slot in range(hold):
        left_ref, lower_ref = block_refs[2 * slot:2 * slot + 2]
        upper = left_ref[0, 0, :half].astype(jnp.float32)
        corner = left_ref[0, 0, half:]
        lower = lower_ref[0, 0].astype(jnp.float32)
        wide = corner.astype(jnp.float32)
        folded = upper * upper + lower * lower + 2.0 * (wide * wide)
        square_sum = square_sum + jnp.sum(jnp.sum(folded, axis=0, keepdims=True), axis=1, keepdims=True)
        diagonal = jnp.sum(jnp.where(row_ids == col_ids, lower, 0.0), axis=0, keepdims=True)
        mixed = jnp.where(row_ids >= col_ids, upper, lower).astype(jnp.bfloat16)
        stripes = [corner[:, c * LANE:(c + 1) * LANE] for c in range(chunks)]
        stripes += [mixed[:, c * LANE:(c + 1) * LANE] for c in range(chunks)]
        per_stripe = half // depth
        for piece in range(pieces):
            stripe, place = piece // per_stripe, piece % per_stripe
            packed_ref[piece, slot * depth:(slot + 1) * depth] = (
                stripes[stripe][place * depth:(place + 1) * depth]
            )
        for c in range(chunks):
            line = diagonal[:, c * LANE:(c + 1) * LANE]
            info = jnp.where(info_row == slot * chunks + c, line, info)
    tail = info_row == hold * chunks
    values = parts_of(square_sum, SQUARE_PARTS)
    for slot in range(hold):
        owner = target_ref[0, slot]
        place = lax.rem(owner, col_count) * row_count + lax.div(owner, col_count)
        place = jnp.zeros((1, 1), jnp.float32) + place.astype(jnp.float32)
        values += parts_of(place, NAME_PARTS)
    for place, value in enumerate(values):
        info = jnp.where(tail & (info_col == place), value.astype(jnp.float32), info)
    info = info.astype(jnp.bfloat16)
    for piece in range(pieces):
        packed_ref[piece, hold * depth:] = info


def pack(factors, target, row_count, col_count):
    hold, width = factors.shape[1], factors.shape[2]
    pieces = row_count * col_count
    depth = width * width // 2 // LANE // pieces
    half = width // 2
    in_specs = [pl.BlockSpec(memory_space=pltpu.SMEM)]
    for slot in range(hold):
        in_specs.append(pl.BlockSpec((1, 1, width, half), lambda i, slot=slot: (0, slot, 0, 0)))
        in_specs.append(pl.BlockSpec((1, 1, half, half), lambda i, slot=slot: (0, slot, 1, 1)))
    return pl.pallas_call(
        functools.partial(pack_kernel, row_count, col_count),
        out_shape=pltpu.VMEM((pieces, hold * depth + INFO_ROWS, LANE), jnp.bfloat16),
        grid=(1,),
        in_specs=in_specs,
        out_specs=pl.BlockSpec(memory_space=pltpu.VMEM),
        name="pack",
    )(target.T, *([factors] * (2 * hold)))


def select_kernel(
    hold, row_count, col_count, width, pieces_ref, chosen_ref, param_ref,
    count_ref, table_ref,
):
    owners, depth = chosen_ref.shape[0], chosen_ref.shape[2]
    rows = hold * depth
    half_lines = width // 2 // LANE
    info = pieces_ref[:, rows:rows + INFO_ROWS].astype(jnp.float32)
    tail = info[:, hold * half_lines]
    names = [tail]
    for part in range(1, NAME_PARTS):
        names.append(pltpu.roll(tail, LANE - part, 1))
    places = sum(names).astype(jnp.int32)
    for owner in range(owners):
        count_ref[owner] = 0
    for device in range(owners):
        source = (device % col_count) * row_count + device // col_count
        for part in range(hold):
            owner = places[source, SQUARE_PARTS + part * NAME_PARTS]
            slot = count_ref[owner]
            count_ref[owner] = slot + 1
            table_ref[owner, slot] = source * hold + part
            chosen_ref[owner, slot] = pieces_ref[source, part * depth:(part + 1) * depth]
    me = lax.axis_index("col") * row_count + lax.axis_index("row")
    source_ids = lax.broadcasted_iota(jnp.int32, (owners, LANE), 0)
    lanes = lax.broadcasted_iota(jnp.int32, (owners, LANE), 1)
    squares = jnp.where(lanes < SQUARE_PARTS, tail, 0.0)
    for slot in range(CAP):
        valid = slot < count_ref[me]
        code = jnp.where(valid, table_ref[me, slot], 0)
        source, part = lax.div(code, hold), lax.rem(code, hold)
        same_row = lax.rem(source_ids, row_count) == lax.rem(source, row_count)
        total = jnp.sum(
            jnp.sum(jnp.where(same_row, squares, 0.0), axis=0, keepdims=True), axis=1, keepdims=True
        )
        scale = 2.0 * jnp.sqrt(total / (col_count * hold * width))
        inverse = 1.0 / scale
        gain = lax.rsqrt(jnp.sqrt(scale))
        here = pieces_ref[source, rows:rows + INFO_ROWS].astype(jnp.float32)
        diagonal = here[:half_lines]
        for other in range(1, hold):
            lines = here[other * half_lines:(other + 1) * half_lines]
            diagonal = jnp.where(part == other, lines, diagonal)
        param_ref[slot, :half_lines] = diagonal
        one = jnp.zeros((1, LANE), jnp.float32)
        param_ref[slot, half_lines:half_lines + 1] = one + inverse
        param_ref[slot, half_lines + 1:half_lines + 2] = jnp.where(valid, one + gain, 0.0)


def select(pieces, hold, row_count, col_count, width):
    owners = pieces.shape[0]
    depth = (pieces.shape[1] - INFO_ROWS) // hold
    return pl.pallas_call(
        functools.partial(select_kernel, hold, row_count, col_count, width),
        out_shape=(
            pltpu.VMEM((owners, CAP, depth, LANE), pieces.dtype),
            pltpu.VMEM((CAP, INFO_ROWS, LANE), jnp.float32),
        ),
        in_specs=[pl.BlockSpec(memory_space=pltpu.VMEM)],
        out_specs=(
            pl.BlockSpec(memory_space=pltpu.VMEM),
            pl.BlockSpec(memory_space=pltpu.VMEM),
        ),
        scratch_shapes=[
            pltpu.SMEM((owners,), jnp.int32),
            pltpu.SMEM((owners, CAP), jnp.int32),
        ],
        name="select",
    )(pltpu.with_memory_space_constraint(pieces, pltpu.VMEM))


def split(value):
    high = value.astype(jnp.bfloat16)
    return high, (value - high.astype(jnp.float32)).astype(jnp.bfloat16)


def dot(left, right):
    return jnp.dot(left, right, preferred_element_type=jnp.float32)


def root_kernel(param_ref, packed_ref, out_ref, made_ref, block_ref, high_ref, low_ref, sem):
    count, width = out_ref.shape[0], out_ref.shape[1]
    half = width // 2
    chunks = half // LANE
    full, top, bottom = slice(0, width), slice(0, half), slice(half, width)
    tiles = ((top, top), (bottom, top), (bottom, bottom))
    row_ids = lax.broadcasted_iota(jnp.int32, (half, half), 0)
    col_ids = lax.broadcasted_iota(jnp.int32, (half, half), 1)
    eye = row_ids == col_ids
    slots = range(count)

    def add_eye(values, scalar):
        there = jnp.where(eye, scalar, 0.0)
        return values[0] + there, values[1], values[2] + there

    def store(slot, place, values):
        for tile, value in zip(tiles, values):
            high, low = split(value)
            high_ref[slot, place, tile[0], tile[1]] = high
            low_ref[slot, place, tile[0], tile[1]] = low
            if tile == (bottom, top):
                high_ref[slot, place, top, bottom] = high.T
                low_ref[slot, place, top, bottom] = low.T

    def dots(left, right):
        def some(rows, cols):
            return dot(
                jnp.concatenate([part(rows, full) for part in left], axis=1),
                jnp.concatenate([part(full, cols) for part in right], axis=0),
            )

        left_half = some(full, top)
        return left_half[top], left_half[bottom], some(bottom, bottom)

    def at(ref, *place):
        return lambda rows, cols: ref[place + (rows, cols)]

    def product(slot, left, right):
        high, low = at(high_ref, slot, left), at(low_ref, slot, left)
        return dots(
            [high, low, high],
            [at(high_ref, slot, right), at(high_ref, slot, right), at(low_ref, slot, right)],
        )

    def square_of(slot, place):
        high, low = at(high_ref, slot, place), at(low_ref, slot, place)
        main = dots([high], [high])
        cross = dot(high(full, full), low(full, full)).astype(jnp.bfloat16)
        flipped = [cross[top, top].T, cross[top, bottom].T, cross[bottom, bottom].T]
        return [
            value + (cross[tile[0], tile[1]].astype(jnp.float32) + other.astype(jnp.float32))
            for value, tile, other in zip(main, tiles, flipped)
        ]

    def by_block(slot, left):
        block = at(block_ref, slot)
        return dots([at(high_ref, slot, left), at(low_ref, slot, left)], [block, block])

    def block_tiles(slot):
        return [block_ref[slot, rows, cols].astype(jnp.float32) for rows, cols in tiles]

    inverses = [param_ref[slot, chunks:chunks + 1, :1] for slot in slots]
    gains = [param_ref[slot, chunks + 1:chunks + 2, :1] for slot in slots]
    for slot in slots:
        lines = packed_ref[:, slot].reshape(-1, LANE)

        def square(place):
            return jnp.concatenate(
                [lines[(place + c) * half:(place + c + 1) * half] for c in range(chunks)], axis=1
            )

        corner = square(0)
        mixed = square(chunks)
        turned = mixed.T.astype(jnp.float32)
        mixed = mixed.astype(jnp.float32)
        upper = jnp.where(row_ids >= col_ids, mixed, turned)
        lower = jnp.where(row_ids < col_ids, mixed, turned)
        diagonal = jnp.concatenate([param_ref[slot, c:c + 1] for c in range(chunks)], axis=1)
        lower = jnp.where(eye, diagonal, lower)
        block_ref[slot, top, top] = upper.astype(jnp.bfloat16)
        block_ref[slot, bottom, top] = corner
        block_ref[slot, top, bottom] = corner.T
        block_ref[slot, bottom, bottom] = lower.astype(jnp.bfloat16)
        scaled = [(0.25 * inverses[slot]) * tile for tile in block_tiles(slot)]
        squared = dots([at(block_ref, slot)], [at(block_ref, slot)])
        factor = 0.0625 * inverses[slot] * inverses[slot]
        store(
            slot, 0, add_eye([factor * b - 2.5 * a for a, b in zip(scaled, squared)], 1.5625)
        )
    def tile_sum(slot, place):
        return [
            high_ref[slot, place, rows, cols].astype(jnp.float32)
            + low_ref[slot, place, rows, cols].astype(jnp.float32)
            for rows, cols in tiles
        ]

    second = -0.5 * LINEAR * LINEAR
    third = -LINEAR * second
    pairs = []
    for slot in slots:
        turned = by_block(slot, 0)
        squares = tile_sum(slot, 0)
        scaled = [(0.25 * inverses[slot]) * tile for tile in block_tiles(slot)]
        near = [
            (1.25 + LINEAR) * b - (0.25 * inverses[slot]) * c - second * a
            for a, b, c in zip(scaled, squares, turned)
        ]
        store(slot, 1, add_eye(near, 1.25 * second + third))
        from_square = second * second + 2.0 * LINEAR * third
        from_step = 2.0 * second * third - 1.25
        rest = [from_step * a - from_square * b for a, b in zip(scaled, squares)]
        pairs.append(add_eye(rest, -1.25 * from_step - third * third))
    for slot in slots:
        store(slot, 0, [a + b for a, b in zip(square_of(slot, 1), pairs[slot])])
    for slot in slots:
        store(slot, 1, square_of(slot, 0))
    for slot in slots:
        store(slot, 2, square_of(slot, 1))
    for slot in slots:
        tail = by_block(slot, 2)
        store(slot, 1, add_eye([-(0.25 * inverses[slot]) * tile for tile in tail], 1.25))
    copies = []

    def send(slot, place, rows):
        span = pl.ds(rows.start, half)
        copies.append(
            pltpu.make_async_copy(made_ref.at[slot, span], out_ref.at[slot, span], sem.at[slot, place])
        )
        copies[-1].start()

    def last_product(slot, rows, cols):
        high, low = at(high_ref, slot, 0), at(low_ref, slot, 0)
        other, small = at(high_ref, slot, 1), at(low_ref, slot, 1)
        return dot(
            jnp.concatenate([part(rows, full) for part in (high, low, high)], axis=1),
            jnp.concatenate([part(full, cols) for part in (other, other, small)], axis=0),
        )

    for slot in slots:
        valid = gains[slot] > 0.0
        lower = jnp.where(valid, last_product(slot, bottom, full) * gains[slot], 0.0)
        made_ref[slot, bottom, full] = lower
        send(slot, 0, bottom)
        upper = jnp.where(valid, last_product(slot, top, top) * gains[slot], 0.0)
        made_ref[slot, top, top] = upper
        made_ref[slot, top, bottom] = lower[:, top].T
        send(slot, 1, top)
    for copy in copies:
        copy.wait()


def root(params, packed, width):
    count = packed.shape[1]
    return pl.pallas_call(
        root_kernel,
        out_shape=jax.ShapeDtypeStruct((count, width, width), jnp.float32),
        in_specs=[
            pl.BlockSpec(memory_space=pltpu.VMEM),
            pl.BlockSpec(memory_space=pltpu.VMEM),
        ],
        out_specs=pl.BlockSpec(memory_space=pl.ANY),
        scratch_shapes=[
            pltpu.VMEM((count, width, width), jnp.float32),
            pltpu.VMEM((count, width, width), jnp.bfloat16),
            pltpu.VMEM((count, 3, width, width), jnp.bfloat16),
            pltpu.VMEM((count, 3, width, width), jnp.bfloat16),
            pltpu.SemaphoreType.DMA((count, 2)),
        ],
        compiler_params=pltpu.CompilerParams(

        ),
        cost_estimate=pl.CostEstimate(
            flops=26 * count * width ** 3,
            bytes_accessed=5 * count * width * width,
            transcendentals=0,
        ),
        name="root",
    )(
        pltpu.with_memory_space_constraint(params, pltpu.VMEM),
        pltpu.with_memory_space_constraint(packed, pltpu.VMEM),
    )


def shards(factors, target):
    row_count, col_count = lax.axis_size("row"), lax.axis_size("col")
    hold, width = factors.shape[1], factors.shape[2]
    packed = pack(factors, target, row_count, col_count)
    pieces = lax.all_to_all(packed, RING, split_axis=0, concat_axis=0, tiled=True)
    chosen, params = select(pieces, hold, row_count, col_count, width)
    landed = lax.all_to_all(chosen, RING, split_axis=0, concat_axis=0, tiled=True)
    return root(params, landed, width)[None]


def solution(mesh):
    return jax.shard_map(
        shards,
        mesh=mesh,
        in_specs=(P(AXES, None, None, None), P(AXES, None)),
        out_specs=P(AXES, None, None, None),
        check_vma=False,
    )
```
